128 devices in a mesh: lat: 16 (over y, x), lev: 8 (over z, core).
Axes of the slice: x: 4, y: 4, z: 4, core: 2. Of those that a mesh axis runs over, the one named last changes fastest.
Arguments:
- activations: bfloat16 [176, 819200], P(None, ('lat', 'lev')), may hold values from -6 to 6
- out_cotangent: bfloat16 [176, 819200], P(None, ('lat', 'lev')), may hold values from -6 to 6
- weight_in: bfloat16 [176, 384], replicated, may hold values from -0.4375 to 0.4375
- weight_mid: bfloat16 [384, 384], replicated, may hold values from -0.3125 to 0.3125
- weight_out: bfloat16 [176, 384], replicated, may hold values from -0.3125 to 0.3125
- legendre: bfloat16 [640, 320, 640], P(('lat', 'lev')), may hold values from -0.25 to 0.25
- level_inverse: bfloat16 [88, 88, 640], replicated, may hold values from -0.625 to 0.625
- wave_order: int32 [640], replicated, may hold values from 0 to 639, each once
Outputs:
- grad_input: float32 [176, 384], replicated
- grad_middle: float32 [384, 384], replicated
- grad_output: float32 [176, 384], replicated
- grid_cotangent: float32 [176, 640, 1280], P(None, ('lat', 'lev'))
The draws below stay inside these ranges and needn't reach their ends.
Inputs may be any that keep to these rules, and one draw needn't show every extreme that they name: wave_order is a permutation of 0 to 639; the device at index d of lat and lev taken together (lat major) holds the d-th block of slots of legendre.
All inputs are finite; a program needn't handle non-finite values.
Results may differ from the reference program's by a relative error of at most 0.017.
Values may be sent and summed in bfloat16 or wider, within the bound.
No kernel may reach another device: no remote copies, remote signals or barrier semaphores. Data moves between devices by JAX's collectives and lax.ppermute only.
A program may use at most 192 MiB of HBM per device.

```python
import math
from functools import partial
import jax
import jax.numpy as jnp
from jax import lax

NLAT = 640
NLON = 1280
L = 88
H = 384
M = 640
F = 176
NDEG = 640
LATB = 40
LONB = 160
COLS = 819200
N_LAT = 16
N_LEV = 8


def steps_of(key, dims, shards, least, top_value):
    def one(position, blocks):
        draws = jax.random.uniform(jax.random.fold_in(jax.random.fold_in(key, 6), position), (blocks,), jnp.float32, least / len(shards), top_value / len(shards))
        return jnp.repeat(jnp.exp(draws), dims[position] // blocks).reshape((-1,) + (1,) * (len(dims) - position - 1))

    level = one(*shards[0])
    for cut in shards[1:]:
        level = level * one(*cut)
    return level


def bell_draw(key, extent, deviation, most, shards=(), kind=jnp.bfloat16):
    values = deviation * jax.random.normal(key, extent, jnp.float32)
    if shards:
        values = values * steps_of(key, extent, shards, -0.22, 0.18)
    return jnp.clip(values, -most, most).astype(kind)


def setup_inputs(seed: int = 0) -> dict:
    splits = jax.random.split(jax.random.key(seed), 9)
    return {
        "activations": bell_draw(splits[0], (F, COLS), 1.0, 6.0, ((1, 128),)),
        "out_cotangent": bell_draw(splits[1], (F, COLS), 1.0, 6.0, ((1, 128),)),
        "weight_in": bell_draw(splits[2], (F, H), F ** -0.5, 0.4375),
        "weight_mid": bell_draw(splits[3], (H, H), H ** -0.5, 0.3125),
        "weight_out": bell_draw(splits[4], (F, H), H ** -0.5, 0.3125),
        "legendre": bell_draw(splits[5], (M, NLAT // 2, NDEG), NLAT ** -0.5, 0.25, ((0, 128),)),
        "level_inverse": bell_draw(splits[6], (L, L, NDEG), L ** -0.5, 0.625),
        "wave_order": jax.random.permutation(splits[7], M).astype(jnp.int32),
    }


def silu_slope(values):
    sigmoid = jax.nn.sigmoid(values)
    return sigmoid * (1.0 + values * (1.0 - sigmoid))

def column_block(blocks, weight_in, weight_mid, weight_out):
    inputs, cotangents = blocks
    pre_first = jnp.dot(weight_in.T, inputs, preferred_element_type=jnp.float32)
    hidden_first = jax.nn.silu(pre_first).astype(jnp.bfloat16)
    pre_second = jnp.dot(weight_mid.T, hidden_first, preferred_element_type=jnp.float32)
    hidden_second = jax.nn.silu(pre_second).astype(jnp.bfloat16)
    back_second = jnp.dot(weight_out.T, cotangents, preferred_element_type=jnp.float32)
    delta_second = (back_second * silu_slope(pre_second)).astype(jnp.bfloat16)
    back_first = jnp.dot(weight_mid, delta_second, preferred_element_type=jnp.float32)
    delta_first = (back_first * silu_slope(pre_first)).astype(jnp.bfloat16)
    grid_part = jnp.dot(weight_in, delta_first, preferred_element_type=jnp.float32).astype(jnp.bfloat16)
    grad_first = jnp.dot(inputs, delta_first.T, preferred_element_type=jnp.float32)
    grad_second = jnp.dot(hidden_first, delta_second.T, preferred_element_type=jnp.float32)
    grad_third = jnp.dot(cotangents, hidden_second.T, preferred_element_type=jnp.float32)
    return (grid_part, grad_first, grad_second, grad_third)

def spectral_block(pieces, level_inverse):
    fourier, legendre_part, wave_local = pieces
    half_lat = NLAT // 2
    widened = fourier.astype(jnp.float32)
    north_rows = widened[..., :half_lat]
    south_rows = widened[..., half_lat:][..., ::-1]
    paired = jnp.stack([north_rows + south_rows, north_rows - south_rows]).astype(jnp.bfloat16)
    table_wide = legendre_part.astype(jnp.float32)
    result = jnp.einsum('ersfj,sjl->serfl', paired.astype(jnp.float32), table_wide)
    degree = jnp.arange(NDEG, dtype=jnp.int32)
    even_mask = (degree[None, :] + wave_local[:, None]) % 2 == 0
    keep_mask = degree[None, :] >= wave_local[:, None]
    even_wide = even_mask[:, None, None, :]
    coeffs = jnp.where(even_wide, result[:, 0], result[:, 1])
    coeffs = jnp.where(keep_mask[:, None, None, :], coeffs, 0.0).astype(jnp.bfloat16)
    slot_total = coeffs.shape[0]
    stacked = coeffs.reshape(slot_total, 2, 2, L, NDEG).astype(jnp.float32)
    solved = jnp.einsum('srakl,kil->srail', stacked, level_inverse.astype(jnp.float32))
    solved = solved.reshape(slot_total, 2, F, NDEG).astype(jnp.bfloat16)
    blank = jnp.zeros_like(solved)
    masked_parts = jnp.stack([jnp.where(even_wide, solved, blank), jnp.where(even_wide, blank, solved)])
    synthesized = jnp.einsum('esrfl,sjl->ersfj', masked_parts.astype(jnp.float32), table_wide)
    north_out = synthesized[0] + synthesized[1]
    south_out = synthesized[0] - synthesized[1]
    return jnp.concatenate([north_out, south_out[..., ::-1]], axis=-1).astype(jnp.bfloat16)

def reference(activations, out_cotangent, weight_in, weight_mid, weight_out, legendre, level_inverse, wave_order):
    block_cols = COLS // N_LAT
    blocks_in = activations.reshape(F, N_LAT, block_cols).transpose(1, 0, 2)
    blocks_cotangent = out_cotangent.reshape(F, N_LAT, block_cols).transpose(1, 0, 2)
    mapped = lax.map(partial(column_block, weight_in=weight_in, weight_mid=weight_mid, weight_out=weight_out), (blocks_in, blocks_cotangent))
    flat_grid = mapped[0].transpose(1, 0, 2).reshape(F, N_LAT, N_LEV, LATB, LONB)
    grid_input = flat_grid.transpose(0, 1, 3, 2, 4).reshape(F, NLAT, NLON)
    grad_scale = 1.0 / math.sqrt(NLAT * NLON)
    grad_input = lax.optimization_barrier(jnp.sum(mapped[1], axis=0)) * grad_scale
    grad_middle = lax.optimization_barrier(jnp.sum(mapped[2], axis=0)) * grad_scale
    grad_output = lax.optimization_barrier(jnp.sum(mapped[3], axis=0)) * grad_scale
    spectrum = jnp.fft.rfft(grid_input.astype(jnp.float32), axis=2) / math.sqrt(NLON)
    picked = jnp.take(spectrum, wave_order, axis=2)
    fourier = jnp.stack([picked.real, picked.imag]).transpose(0, 3, 1, 2).astype(jnp.bfloat16)
    group_size = M // N_LAT
    grouped = fourier.reshape(2, N_LAT, group_size, F, NLAT).transpose(1, 0, 2, 3, 4)
    tables = legendre.reshape(N_LAT, group_size, NLAT // 2, NDEG)
    wave_groups = wave_order.reshape(N_LAT, group_size)
    zonal_rows = lax.map(partial(spectral_block, level_inverse=level_inverse), (grouped, tables, wave_groups))
    zonal_rows = zonal_rows.transpose(1, 0, 2, 3, 4).reshape(2, M, F, NLAT).astype(jnp.float32)
    complex_rows = zonal_rows[0] + 1j * zonal_rows[1]
    full_spectrum = jnp.zeros((NLON // 2 + 1, F, NLAT), complex_rows.dtype).at[wave_order].set(complex_rows)
    grid_cotangent = (jnp.fft.irfft(full_spectrum, n=NLON, axis=0) * math.sqrt(NLON)).transpose(1, 2, 0)
    return (grad_input, grad_middle, grad_output, grid_cotangent)
```

```python
import math
from functools import partial

import jax
import jax.numpy as jnp
from jax import lax
from jax.experimental import pallas as pl
from jax.experimental.pallas import tpu as pltpu
from jax.sharding import PartitionSpec as P

NLAT = 640
NLON = 1280
LEVELS = 88
FEATURES = 176
HIDDEN = 384
NDEG = 640
HALF = NLAT // 2
SLOTS = 5
WAYS = 128
LONB = 160
LANES = 128
WIDTH = 896
TILES = WIDTH // LANES
DATA_ROWS = 2 * SLOTS * TILES
GRAD_ROWS = 18
ROWS = DATA_ROWS + GRAD_ROWS
COLS = 6400
TILE = 256
STEPS = COLS // TILE
BANK = 24
EVERYWHERE = ("lat", "lev")

VMEM = pl.BlockSpec(memory_space=pltpu.VMEM)
SMEM = pl.BlockSpec(memory_space=pltpu.SMEM)
ANY = pl.BlockSpec(memory_space=pl.ANY)


def mm(left, right):
    return jnp.dot(left, right, preferred_element_type=jnp.float32)


def mm_nt(left, right):
    return lax.dot_general(left, right, (((1,), (1,)), ((), ())), preferred_element_type=jnp.float32)


def mm_tn(left, right):
    return lax.dot_general(left, right, (((0,), (0,)), ((), ())), preferred_element_type=jnp.float32)


def params(mib):
    return pltpu.CompilerParams(vmem_limit_bytes=mib * 1024 * 1024)


def column_kernel(x_ref, c_ref, wi_ref, wm_ref, wo_ref, out_ref, grad_ref, wit, wmt, wot, grid_ref, g1, g2, g3):
    n = pl.program_id(0)

    @pl.when(n == 0)
    def _():
        wit[...] = wi_ref[...].T
        wmt[...] = wm_ref[...].T
        wot[...] = wo_ref[...].T
        g1[...] = jnp.zeros_like(g1)
        g2[...] = jnp.zeros_like(g2)
        g3[...] = jnp.zeros_like(g3)
        grid_ref[SLOTS * FEATURES :, :] = jnp.zeros((WIDTH - SLOTS * FEATURES, NLON), jnp.bfloat16)

    x = x_ref[...]
    c = c_ref[...]
    pre1 = mm(wit[...], x)
    s1 = 0.5 * jnp.tanh(0.5 * pre1) + 0.5
    silu1 = pre1 * s1
    slope1 = s1 + silu1 * (1.0 - s1)
    h1 = silu1.astype(jnp.bfloat16)
    pre2 = mm(wmt[...], h1)
    s2 = 0.5 * jnp.tanh(0.5 * pre2) + 0.5
    silu2 = pre2 * s2
    slope2 = s2 + silu2 * (1.0 - s2)
    h2 = silu2.astype(jnp.bfloat16)
    d2 = (mm(wot[...], c) * slope2).astype(jnp.bfloat16)
    d1 = (mm(wm_ref[...], d2) * slope1).astype(jnp.bfloat16)
    gi = mm(wi_ref[...], d1).astype(jnp.bfloat16)
    g1[...] += mm_nt(x, d1)
    g2[...] += mm_nt(h1, d2)
    g3[...] += mm_nt(c, h2)
    band = n // (NLON // TILE)
    part = n % (NLON // TILE)
    grid_ref[pl.ds(pl.multiple_of(band * FEATURES, 16), FEATURES), pl.ds(pl.multiple_of(part * TILE, TILE), TILE)] = gi

    @pl.when(n == STEPS - 1)
    def _():
        for t in range(TILES):
            out_ref[:, LANES * t : LANES * (t + 1)] = grid_ref[LANES * t : LANES * (t + 1), :].T
        at = 0
        for g in (g1, g2, g3):
            rows = g.shape[0]
            for t in range(HIDDEN // LANES):
                grad_ref[at : at + rows, :] = g[:, LANES * t : LANES * (t + 1)]
                at += rows
        grad_ref[at:, :] = jnp.zeros((GRAD_ROWS * WAYS - at, LANES), jnp.float32)


def columns(x, c, wi, wm, wo):
    block = pl.BlockSpec((FEATURES, TILE), lambda n: (0, n))
    return pl.pallas_call(
        column_kernel,
        grid=(STEPS,),
        in_specs=[block, block] + [pl.BlockSpec(w.shape, lambda n: (0, 0)) for w in (wi, wm, wo)],
        out_specs=[
            pl.BlockSpec((NLON, WIDTH), lambda n: (0, 0)),
            pl.BlockSpec((GRAD_ROWS * WAYS, LANES), lambda n: (0, 0)),
        ],
        out_shape=[
            jax.ShapeDtypeStruct((NLON, WIDTH), jnp.bfloat16),
            jax.ShapeDtypeStruct((GRAD_ROWS * WAYS, LANES), jnp.float32),
        ],
        scratch_shapes=[
            pltpu.VMEM((HIDDEN, FEATURES), jnp.bfloat16),
            pltpu.VMEM((HIDDEN, HIDDEN), jnp.bfloat16),
            pltpu.VMEM((HIDDEN, FEATURES), jnp.bfloat16),
            pltpu.VMEM((WIDTH, NLON), jnp.bfloat16),
            pltpu.VMEM((FEATURES, HIDDEN), jnp.float32),
            pltpu.VMEM((HIDDEN, HIDDEN), jnp.float32),
            pltpu.VMEM((FEATURES, HIDDEN), jnp.float32),
        ],
        compiler_params=params(48),
        name="columns",
    )(x, c, wi, wm, wo)


def wave_kernel(ca_ref, sa_ref, cb_ref, sb_ref, out_ref):
    for s in range(SLOTS):
        rows = slice(WAYS * s, WAYS * (s + 1))
        cb, sb = cb_ref[rows, :], sb_ref[rows, :]
        for a in range(NLON // LANES):
            ca, sa = ca_ref[rows, a : a + 1], sa_ref[rows, a : a + 1]
            cols = slice(LANES * a, LANES * (a + 1))
            out_ref[WAYS * 2 * s : WAYS * (2 * s + 1), cols] = (ca * cb - sa * sb).astype(jnp.bfloat16)
            out_ref[WAYS * (2 * s + 1) : WAYS * (2 * s + 2), cols] = (-(sa * cb + ca * sb)).astype(jnp.bfloat16)


def wave_table(wave_order):
    m = wave_order.reshape(WAYS, SLOTS).T.reshape(NLAT, 1)
    turn = 2.0 * math.pi / NLON
    fine = (m * jnp.arange(LANES, dtype=jnp.int32)[None, :] % NLON).astype(jnp.float32) * turn
    coarse = (m * (LANES * jnp.arange(NLON // LANES, dtype=jnp.int32))[None, :] % NLON).astype(jnp.float32) * turn
    scale = 1.0 / math.sqrt(NLON)
    return pl.pallas_call(
        wave_kernel,
        in_specs=[VMEM] * 4,
        out_specs=VMEM,
        out_shape=jax.ShapeDtypeStruct((NLON, NLON), jnp.bfloat16),
        compiler_params=params(32),
        name="waves",
    )(jnp.cos(coarse), jnp.sin(coarse), jnp.cos(fine) * scale, jnp.sin(fine) * scale)


def legendre_kernel(m_ref, leg_ref, at_ref, as_ref):
    m = m_ref[pl.program_id(0)]
    leg = leg_ref[0]
    row = lax.broadcasted_iota(jnp.int32, (HALF, NLAT), 0)
    col = lax.broadcasted_iota(jnp.int32, (HALF, NLAT), 1)
    lat = 40 * ((col & 127) >> 3) + 8 * (col >> 7) + (col & 7)
    pick = (jnp.where(lat < HALF, lat, NLAT - 1 - lat) == row).astype(jnp.bfloat16)
    full = mm_tn(leg, pick)
    deg = lax.broadcasted_iota(jnp.int32, (NDEG, NLAT), 0)
    col = lax.broadcasted_iota(jnp.int32, (NDEG, NLAT), 1)
    south = (col & 127) >= 64
    full = jnp.where(south & (((deg + m) & 1) == 1), -full, full)
    at_ref[0] = jnp.where(deg >= m, full, 0.0).astype(jnp.bfloat16)
    row = lax.broadcasted_iota(jnp.int32, (NLAT, HALF), 0)
    col = lax.broadcasted_iota(jnp.int32, (NLAT, HALF), 1)
    lat = 5 * (row & 127) + (row >> 7)
    pick = (jnp.where(lat < HALF, lat, NLAT - 1 - lat) == col).astype(jnp.bfloat16)
    full = mm(pick, leg)
    row = lax.broadcasted_iota(jnp.int32, (NLAT, NDEG), 0)
    deg = lax.broadcasted_iota(jnp.int32, (NLAT, NDEG), 1)
    south = (row & 127) >= 64
    full = jnp.where(south & (((deg + m) & 1) == 1), -full, full)
    as_ref[0] = jnp.where(deg >= m, full, 0.0).astype(jnp.bfloat16)


def legendre_tables(wave_local, legendre):
    block = pl.BlockSpec((1, NDEG, NLAT), lambda s, m: (s, 0, 0))
    table = jax.ShapeDtypeStruct((SLOTS, NDEG, NLAT), jnp.bfloat16)
    return pl.pallas_call(
        legendre_kernel,
        grid_spec=pltpu.PrefetchScalarGridSpec(
            num_scalar_prefetch=1,
            grid=(SLOTS,),
            in_specs=[pl.BlockSpec((1, HALF, NDEG), lambda s, m: (s, 0, 0))],
            out_specs=[block, block],
        ),
        out_shape=[table, table],
        compiler_params=params(40),
        name="legendre",
    )(wave_local, legendre)


def pack_out(wide_ref, out_ref):
    def body(p, carry):
        out_ref[p] = wide_ref[pl.ds(pl.multiple_of(ROWS * p, 8), ROWS), :].astype(jnp.bfloat16)
        return carry

    lax.fori_loop(0, WAYS, body, 0, unroll=4)


def unpack_in(in_ref, wide_ref):
    def body(p, carry):
        wide_ref[pl.ds(pl.multiple_of(ROWS * p, 8), ROWS), :] = in_ref[p].astype(jnp.float32)
        return carry

    lax.fori_loop(0, WAYS, body, 0, unroll=4)


def forward_kernel(x_ref, table_ref, grad_ref, out_ref, wide_ref):
    def body(k, carry):
        piece = mm(table_ref[pl.ds(pl.multiple_of(256 * k, 256), 256), :], x_ref[...])
        for h in range(2):
            for t in range(TILES):
                wide_ref[pl.ds((2 * k + h) * TILES + t, WAYS, stride=ROWS), :] = piece[
                    WAYS * h : WAYS * (h + 1), LANES * t : LANES * (t + 1)
                ]
        return carry

    lax.fori_loop(0, SLOTS, body, 0)
    for k in range(GRAD_ROWS):
        wide_ref[pl.ds(DATA_ROWS + k, WAYS, stride=ROWS), :] = grad_ref[WAYS * k : WAYS * (k + 1), :]
    pack_out(wide_ref, out_ref)


def forward(x, table, grad):
    return pl.pallas_call(
        forward_kernel,
        in_specs=[VMEM] * 3,
        out_specs=VMEM,
        out_shape=jax.ShapeDtypeStruct((WAYS, ROWS, LANES), jnp.bfloat16),
        scratch_shapes=[pltpu.VMEM((WAYS * ROWS, LANES), jnp.float32)],
        compiler_params=params(48),
        name="forward",
    )(x, table, grad)


def spectral_kernel(m_ref, in_ref, at_ref, inv_hbm, as_hbm, out_ref, wide_ref, x_ref, bank_ref, inv_ref, as_ref, sums_ref, sems):
    inv_copy = pltpu.make_async_copy(inv_hbm, inv_ref, sems.at[0])
    as_copy = pltpu.make_async_copy(as_hbm, as_ref, sems.at[1])
    inv_copy.start()
    as_copy.start()
    unpack_in(in_ref, wide_ref)
    for k in range(GRAD_ROWS):
        slab = wide_ref[pl.ds(DATA_ROWS + k, WAYS, stride=ROWS), :]
        sums_ref[k : k + 1, :] = jnp.sum(slab, axis=0, keepdims=True)
    lane = lax.broadcasted_iota(jnp.int32, (WAYS, LANES), 1)

    def analyse(s, carry):
        for r in range(2):
            tiles = [wide_ref[pl.ds((2 * s + r) * TILES + t, WAYS, stride=ROWS), :] for t in range(TILES)]
            for g in range(2 * SLOTS):
                t, off = divmod(LEVELS * g, LANES)
                piece = tiles[t]
                if off:
                    piece = pltpu.roll(piece, LANES - off, 1)
                    if off + LEVELS > LANES:
                        piece = jnp.where(lane < LANES - off, piece, pltpu.roll(tiles[t + 1], LANES - off, 1))
                i, a = divmod(g, 2)
                x_ref[WAYS * i : WAYS * (i + 1), LANES * (2 * r + a) : LANES * (2 * r + a + 1)] = piece.astype(jnp.bfloat16)
        y = mm(at_ref[s], x_ref[...])
        for j in range(4):
            bank_ref[pl.ds(4 * s + j, NDEG, stride=BANK), :] = y[:, LANES * j : LANES * (j + 1)]
        return carry

    lax.fori_loop(0, SLOTS, analyse, 0)
    inv_copy.wait()

    def solve(k, carry):
        for u in range(16):
            deg = 16 * k + u
            rows = pl.ds(pl.multiple_of(deg * BANK, 8), BANK)
            bank_ref[rows, :LEVELS] = mm(bank_ref[rows, :LEVELS].astype(jnp.bfloat16), inv_ref[deg])
        return carry

    lax.fori_loop(0, NDEG // 16, solve, 0)
    as_copy.wait()

    def synthesise(s, carry):
        z = jnp.concatenate(
            [bank_ref[pl.ds(4 * s + j, NDEG, stride=BANK), :].astype(jnp.bfloat16) for j in range(4)], axis=1
        )
        weight = jnp.where(m_ref[s] == 0, 1.0, 2.0)
        w = mm(as_ref[s], z) * weight
        for r in range(2):
            tiles = [None] * TILES
            for g in range(2 * SLOTS):
                i, a = divmod(g, 2)
                piece = w[WAYS * i : WAYS * (i + 1), LANES * (2 * r + a) : LANES * (2 * r + a + 1)]
                t, off = divmod(LEVELS * g, LANES)
                if off:
                    piece = pltpu.roll(piece, off, 1)
                tiles[t] = piece if off == 0 else jnp.where(lane < off, tiles[t], piece)
                if off + LEVELS > LANES:
                    tiles[t + 1] = piece
            for t in range(TILES):
                wide_ref[pl.ds((2 * s + r) * TILES + t, WAYS, stride=ROWS), :] = tiles[t]
        return carry

    lax.fori_loop(0, SLOTS, synthesise, 0)
    for k in range(GRAD_ROWS):
        wide_ref[pl.ds(DATA_ROWS + k, WAYS, stride=ROWS), :] = jnp.broadcast_to(sums_ref[k : k + 1, :], (WAYS, LANES))
    pack_out(wide_ref, out_ref)


def spectral(wave_local, arrived, at, inv, synth):
    return pl.pallas_call(
        spectral_kernel,
        in_specs=[SMEM, VMEM, VMEM, ANY, ANY],
        out_specs=VMEM,
        out_shape=jax.ShapeDtypeStruct((WAYS, ROWS, LANES), jnp.bfloat16),
        scratch_shapes=[
            pltpu.VMEM((WAYS * ROWS, LANES), jnp.float32),
            pltpu.VMEM((NLAT, 4 * LANES), jnp.bfloat16),
            pltpu.VMEM((NDEG * BANK, LANES), jnp.float32),
            pltpu.VMEM((NDEG, LEVELS, LEVELS), jnp.bfloat16),
            pltpu.VMEM((SLOTS, NLAT, NDEG), jnp.bfloat16),
            pltpu.VMEM((24, LANES), jnp.float32),
            pltpu.SemaphoreType.DMA((2,)),
        ],
        compiler_params=params(58),
        name="spectral",
    )(wave_local, arrived, at, inv, synth)


def inverse_kernel(in_ref, table_ref, out_ref, g1, g2, g3, wide_ref, rows_ref, grad_ref):
    unpack_in(in_ref, wide_ref)
    for t in range(TILES):
        for c in range(2 * SLOTS):
            slab = wide_ref[pl.ds(TILES * c + t, WAYS, stride=ROWS), :]
            rows_ref[LANES * t : LANES * (t + 1), WAYS * c : WAYS * (c + 1)] = slab.T.astype(jnp.bfloat16)
    for i in range(SLOTS):
        out_ref[i] = mm(rows_ref[FEATURES * i : FEATURES * (i + 1), :], table_ref[...])
    for k in range(GRAD_ROWS):
        grad_ref[WAYS * k : WAYS * (k + 1), :] = wide_ref[pl.ds(DATA_ROWS + k, WAYS, stride=ROWS), :]
    scale = 1.0 / math.sqrt(NLAT * NLON)
    at = 0
    for g in (g1, g2, g3):
        rows = g.shape[0]
        for t in range(HIDDEN // LANES):
            g[:, LANES * t : LANES * (t + 1)] = grad_ref[at : at + rows, :] * scale
            at += rows


def inverse(arrived, table):
    return pl.pallas_call(
        inverse_kernel,
        in_specs=[VMEM] * 2,
        out_specs=[VMEM] * 4,
        out_shape=[
            jax.ShapeDtypeStruct((SLOTS, FEATURES, NLON), jnp.float32),
            jax.ShapeDtypeStruct((FEATURES, HIDDEN), jnp.float32),
            jax.ShapeDtypeStruct((HIDDEN, HIDDEN), jnp.float32),
            jax.ShapeDtypeStruct((FEATURES, HIDDEN), jnp.float32),
        ],
        scratch_shapes=[
            pltpu.VMEM((WAYS * ROWS, LANES), jnp.float32),
            pltpu.VMEM((WIDTH, NLON), jnp.bfloat16),
            pltpu.VMEM((GRAD_ROWS * WAYS, LANES), jnp.float32),
        ],
        compiler_params=params(48),
        name="inverse",
    )(arrived, table)


def swap(array, axis):
    return lax.all_to_all(array, axis, split_axis=0, concat_axis=0, tiled=True)


def on_device(x, c, wi, wm, wo, legendre, level_inverse, wave_order):
    grid, grad = columns(x, c, wi, wm, wo)
    grid, legendre, level_inverse, wave_order = lax.optimization_barrier((grid, legendre, level_inverse, wave_order))
    rows = swap(grid.reshape(8, LONB, WIDTH), "lev").reshape(NLON, WIDTH)
    wave_local = lax.dynamic_slice_in_dim(wave_order, lax.axis_index(EVERYWHERE) * SLOTS, SLOTS)
    table = wave_table(wave_order)
    at, synth = legendre_tables(wave_local, legendre)
    inv = level_inverse.transpose(2, 0, 1)
    arrived = swap(forward(rows, table, grad), EVERYWHERE)
    arrived = swap(spectral(wave_local, arrived, at, inv, synth), EVERYWHERE)
    out, g1, g2, g3 = inverse(arrived, table)
    return g1, g2, g3, out.transpose(1, 0, 2)


def solution(mesh):
    in_specs = (
        P(None, EVERYWHERE),
        P(None, EVERYWHERE),
        P(),
        P(),
        P(),
        P(EVERYWHERE, None, None),
        P(),
        P(),
    )
    out_specs = (P(), P(), P(), P(None, EVERYWHERE, None))
    return jax.shard_map(on_device, mesh=mesh, in_specs=in_specs, out_specs=out_specs, check_vma=False)
```

```python
import math
from functools import partial

import jax
import jax.numpy as jnp
from jax import lax
from jax.experimental import pallas as pl
from jax.experimental.pallas import tpu as pltpu
from jax.sharding import PartitionSpec as P

NLAT = 640
NLON = 1280
LEVELS = 88
FEATURES = 176
HIDDEN = 384
NDEG = 640
HALF = NLAT // 2
SLOTS = 5
WAYS = 128
LONB = 160
LANES = 128
WIDTH = 896
TILES = WIDTH // LANES
DATA_ROWS = 2 * SLOTS * TILES
GRAD_ROWS = 18
ROWS = DATA_ROWS + GRAD_ROWS
COLS = 6400
TILE = 256
STEPS = COLS // NLON
BANK = 25
PITCH = 89
EVERYWHERE = ("lat", "lev")

VMEM = pl.BlockSpec(memory_space=pltpu.VMEM)
SMEM = pl.BlockSpec(memory_space=pltpu.SMEM)
ANY = pl.BlockSpec(memory_space=pl.ANY)


def mm(left, right):
    return jnp.dot(left, right, preferred_element_type=jnp.float32)


def mm_nt(left, right):
    return lax.dot_general(left, right, (((1,), (1,)), ((), ())), preferred_element_type=jnp.float32)


def mm_tn(left, right):
    return lax.dot_general(left, right, (((0,), (0,)), ((), ())), preferred_element_type=jnp.float32)


def params(mib):
    return pltpu.CompilerParams(vmem_limit_bytes=mib * 1024 * 1024)


def column_kernel(x_ref, c_ref, wi_ref, wm_ref, wo_ref, out_ref, grad_ref, wit, wmt, wot, wmh, h1_ref, h2_ref, d1_ref, d2_ref, s1_ref, grid_ref, g1, g2, g3):
    n = pl.program_id(0)

    @pl.when(n == 0)
    def _():
        half = jnp.bfloat16(0.5)
        wit[...] = wi_ref[...].T * half
        wmt[...] = wm_ref[...].T * half
        wot[...] = wo_ref[...].T * half
        wmh[...] = wm_ref[...] * half
        g1[...] = jnp.zeros_like(g1)
        g2[...] = jnp.zeros_like(g2)
        g3[...] = jnp.zeros_like(g3)
        grid_ref[SLOTS * FEATURES :, :] = jnp.zeros((WIDTH - SLOTS * FEATURES, NLON), jnp.bfloat16)

    band = pl.ds(pl.multiple_of(n * FEATURES, 16), FEATURES)
    tiles = [slice(TILE * t, TILE * (t + 1)) for t in range(NLON // TILE)]
    parts = [slice(384 * t, 384 * (t + 1)) for t in range(HIDDEN // 384)]
    for cols in tiles:
        for rows in parts:
            u = mm(wit[rows, :], x_ref[:, cols])
            tanh = jnp.tanh(u)
            p = 1.0 + tanh
            h1_ref[rows, cols] = (u * p).astype(jnp.bfloat16)
            s1_ref[rows, cols] = p * (1.0 + u * (1.0 - tanh))
    for cols in tiles:
        for rows in parts:
            u = mm(wmt[rows, :], h1_ref[:, cols])
            back = mm(wot[rows, :], c_ref[:, cols])
            tanh = jnp.tanh(u)
            p = 1.0 + tanh
            h2_ref[rows, cols] = (u * p).astype(jnp.bfloat16)
            d2_ref[rows, cols] = (back * (p * (1.0 + u * (1.0 - tanh)))).astype(jnp.bfloat16)
    for cols in tiles:
        for rows in parts:
            d1_ref[rows, cols] = (mm(wmh[rows, :], d2_ref[:, cols]) * s1_ref[rows, cols]).astype(jnp.bfloat16)
    for cols in tiles:
        grid_ref[band, cols] = mm(wi_ref[...], d1_ref[:, cols]).astype(jnp.bfloat16)
    g1[...] += mm_nt(x_ref[...], d1_ref[...])
    g2[...] += mm_nt(h1_ref[...], d2_ref[...])
    g3[...] += mm_nt(c_ref[...], h2_ref[...])

    @pl.when(n == STEPS - 1)
    def _():
        for t in range(TILES):
            out_ref[:, LANES * t : LANES * (t + 1)] = grid_ref[LANES * t : LANES * (t + 1), :].T
        at = 0
        for g in (g1, g2, g3):
            rows = g.shape[0]
            for t in range(HIDDEN // LANES):
                grad_ref[at : at + rows, :] = g[:, LANES * t : LANES * (t + 1)]
                at += rows
        grad_ref[at:, :] = jnp.zeros((GRAD_ROWS * WAYS - at, LANES), jnp.float32)


def columns(x, c, wi, wm, wo):
    block = pl.BlockSpec((FEATURES, NLON), lambda n: (0, n))
    kept = pltpu.VMEM((HIDDEN, NLON), jnp.bfloat16)
    return pl.pallas_call(
        column_kernel,
        grid=(STEPS,),
        in_specs=[block, block] + [pl.BlockSpec(w.shape, lambda n: (0, 0)) for w in (wi, wm, wo)],
        out_specs=[
            pl.BlockSpec((NLON, WIDTH), lambda n: (0, 0)),
            pl.BlockSpec((GRAD_ROWS * WAYS, LANES), lambda n: (0, 0)),
        ],
        out_shape=[
            jax.ShapeDtypeStruct((NLON, WIDTH), jnp.bfloat16),
            jax.ShapeDtypeStruct((GRAD_ROWS * WAYS, LANES), jnp.float32),
        ],
        scratch_shapes=[
            pltpu.VMEM((HIDDEN, FEATURES), jnp.bfloat16),
            pltpu.VMEM((HIDDEN, HIDDEN), jnp.bfloat16),
            pltpu.VMEM((HIDDEN, FEATURES), jnp.bfloat16),
            pltpu.VMEM((HIDDEN, HIDDEN), jnp.bfloat16),
            kept,
            kept,
            kept,
            kept,
            pltpu.VMEM((HIDDEN, NLON), jnp.float32),
            pltpu.VMEM((WIDTH, NLON), jnp.bfloat16),
            pltpu.VMEM((FEATURES, HIDDEN), jnp.float32),
            pltpu.VMEM((HIDDEN, HIDDEN), jnp.float32),
            pltpu.VMEM((FEATURES, HIDDEN), jnp.float32),
        ],
        compiler_params=params(48),
        name="columns",
    )(x, c, wi, wm, wo)


def wave_kernel(ca_ref, sa_ref, cb_ref, sb_ref, out_ref):
    for s in range(SLOTS):
        rows = slice(WAYS * s, WAYS * (s + 1))
        cb, sb = cb_ref[rows, :], sb_ref[rows, :]
        for a in range(NLON // LANES):
            ca, sa = ca_ref[rows, a : a + 1], sa_ref[rows, a : a + 1]
            cols = slice(LANES * a, LANES * (a + 1))
            out_ref[WAYS * 2 * s : WAYS * (2 * s + 1), cols] = (ca * cb - sa * sb).astype(jnp.bfloat16)
            out_ref[WAYS * (2 * s + 1) : WAYS * (2 * s + 2), cols] = (-(sa * cb + ca * sb)).astype(jnp.bfloat16)


def wave_table(wave_order):
    m = wave_order.reshape(WAYS, SLOTS).T.reshape(NLAT, 1)
    turn = 2.0 * math.pi / NLON
    fine = (m * jnp.arange(LANES, dtype=jnp.int32)[None, :] % NLON).astype(jnp.float32) * turn
    coarse = (m * (LANES * jnp.arange(NLON // LANES, dtype=jnp.int32))[None, :] % NLON).astype(jnp.float32) * turn
    scale = 1.0 / math.sqrt(NLON)
    return pl.pallas_call(
        wave_kernel,
        in_specs=[VMEM] * 4,
        out_specs=VMEM,
        out_shape=jax.ShapeDtypeStruct((NLON, NLON), jnp.bfloat16),
        compiler_params=params(32),
        name="waves",
    )(jnp.cos(coarse), jnp.sin(coarse), jnp.cos(fine) * scale, jnp.sin(fine) * scale)


def legendre_kernel(m_ref, leg_ref, at_ref, as_ref):
    m = m_ref[pl.program_id(0)]
    leg = leg_ref[0]
    row = lax.broadcasted_iota(jnp.int32, (HALF, NLAT), 0)
    col = lax.broadcasted_iota(jnp.int32, (HALF, NLAT), 1)
    lat = 40 * ((col & 127) >> 3) + 8 * (col >> 7) + (col & 7)
    pick = (jnp.where(lat < HALF, lat, NLAT - 1 - lat) == row).astype(jnp.bfloat16)
    full = mm_tn(leg, pick)
    deg = lax.broadcasted_iota(jnp.int32, (NDEG, NLAT), 0)
    col = lax.broadcasted_iota(jnp.int32, (NDEG, NLAT), 1)
    south = (col & 127) >= 64
    full = jnp.where(south & (((deg + m) & 1) == 1), -full, full)
    at_ref[0] = jnp.where(deg >= m, full, 0.0).astype(jnp.bfloat16)
    row = lax.broadcasted_iota(jnp.int32, (NLAT, HALF), 0)
    col = lax.broadcasted_iota(jnp.int32, (NLAT, HALF), 1)
    lat = 5 * (row & 127) + (row >> 7)
    pick = (jnp.where(lat < HALF, lat, NLAT - 1 - lat) == col).astype(jnp.bfloat16)
    full = mm(pick, leg)
    row = lax.broadcasted_iota(jnp.int32, (NLAT, NDEG), 0)
    deg = lax.broadcasted_iota(jnp.int32, (NLAT, NDEG), 1)
    south = (row & 127) >= 64
    full = jnp.where(south & (((deg + m) & 1) == 1), -full, full)
    as_ref[0] = jnp.where(deg >= m, full, 0.0).astype(jnp.bfloat16)


def legendre_tables(wave_local, legendre):
    block = pl.BlockSpec((1, NDEG, NLAT), lambda s, m: (s, 0, 0))
    table = jax.ShapeDtypeStruct((SLOTS, NDEG, NLAT), jnp.bfloat16)
    return pl.pallas_call(
        legendre_kernel,
        grid_spec=pltpu.PrefetchScalarGridSpec(
            num_scalar_prefetch=1,
            grid=(SLOTS,),
            in_specs=[pl.BlockSpec((1, HALF, NDEG), lambda s, m: (s, 0, 0))],
            out_specs=[block, block],
        ),
        out_shape=[table, table],
        compiler_params=params(40),
        name="legendre",
    )(wave_local, legendre)


def pack_out(wide_ref, out_ref):
    def body(p, carry):
        out_ref[p] = wide_ref[pl.ds(PITCH * p, ROWS), :].astype(jnp.bfloat16)
        return carry

    lax.fori_loop(0, WAYS, body, 0, unroll=4)


def unpack_in(in_ref, wide_ref):
    def body(p, carry):
        wide_ref[pl.ds(PITCH * p, ROWS), :] = in_ref[p].astype(jnp.float32)
        return carry

    lax.fori_loop(0, WAYS, body, 0, unroll=4)


def forward_kernel(x_ref, table_ref, grad_ref, out_ref, wide_ref):
    def body(k, carry):
        piece = mm(table_ref[pl.ds(pl.multiple_of(256 * k, 256), 256), :], x_ref[...])
        for h in range(2):
            for t in range(TILES):
                wide_ref[pl.ds((2 * k + h) * TILES + t, WAYS, stride=PITCH), :] = piece[
                    WAYS * h : WAYS * (h + 1), LANES * t : LANES * (t + 1)
                ]
        return carry

    lax.fori_loop(0, SLOTS, body, 0)
    for k in range(GRAD_ROWS):
        wide_ref[pl.ds(DATA_ROWS + k, WAYS, stride=PITCH), :] = grad_ref[WAYS * k : WAYS * (k + 1), :]
    pack_out(wide_ref, out_ref)


def forward(x, table, grad):
    return pl.pallas_call(
        forward_kernel,
        in_specs=[VMEM] * 3,
        out_specs=VMEM,
        out_shape=jax.ShapeDtypeStruct((WAYS, ROWS, LANES), jnp.bfloat16),
        scratch_shapes=[pltpu.VMEM((WAYS * PITCH, LANES), jnp.float32)],
        compiler_params=params(48),
        name="forward",
    )(x, table, grad)


def spectral_kernel(m_ref, in_ref, at_ref, inv_hbm, as_hbm, out_ref, wide_ref, x_ref, bank_ref, inv_ref, as_ref, sums_ref, sems):
    inv_copy = pltpu.make_async_copy(inv_hbm, inv_ref, sems.at[0])
    as_copy = pltpu.make_async_copy(as_hbm, as_ref, sems.at[1])
    inv_copy.start()
    as_copy.start()
    unpack_in(in_ref, wide_ref)
    for k in range(GRAD_ROWS):
        slab = wide_ref[pl.ds(DATA_ROWS + k, WAYS, stride=PITCH), :]
        sums_ref[k : k + 1, :] = jnp.sum(slab, axis=0, keepdims=True)
    lane = lax.broadcasted_iota(jnp.int32, (WAYS, LANES), 1)

    def analyse(s, carry):
        for r in range(2):
            tiles = [wide_ref[pl.ds((2 * s + r) * TILES + t, WAYS, stride=PITCH), :] for t in range(TILES)]
            for g in range(2 * SLOTS):
                t, off = divmod(LEVELS * g, LANES)
                piece = tiles[t]
                if off:
                    piece = pltpu.roll(piece, LANES - off, 1)
                    if off + LEVELS > LANES:
                        piece = jnp.where(lane < LANES - off, piece, pltpu.roll(tiles[t + 1], LANES - off, 1))
                i, a = divmod(g, 2)
                x_ref[WAYS * i : WAYS * (i + 1), LANES * (2 * r + a) : LANES * (2 * r + a + 1)] = piece.astype(jnp.bfloat16)
        y = mm(at_ref[s], x_ref[...])
        for j in range(4):
            bank_ref[pl.ds(4 * s + j, NDEG, stride=BANK), :] = y[:, LANES * j : LANES * (j + 1)]
        return carry

    lax.fori_loop(0, SLOTS, analyse, 0)
    inv_copy.wait()

    def solve(k, carry):
        for u in range(16):
            deg = 16 * k + u
            rows = pl.ds(deg * BANK, 24)
            bank_ref[rows, :LEVELS] = mm(bank_ref[rows, :LEVELS].astype(jnp.bfloat16), inv_ref[deg])
        return carry

    lax.fori_loop(0, NDEG // 16, solve, 0)
    as_copy.wait()

    def synthesise(s, carry):
        z = jnp.concatenate(
            [bank_ref[pl.ds(4 * s + j, NDEG, stride=BANK), :].astype(jnp.bfloat16) for j in range(4)], axis=1
        )
        weight = jnp.where(m_ref[s] == 0, 1.0, 2.0)
        w = mm(as_ref[s], z) * weight
        for r in range(2):
            tiles = [None] * TILES
            for g in range(2 * SLOTS):
                i, a = divmod(g, 2)
                piece = w[WAYS * i : WAYS * (i + 1), LANES * (2 * r + a) : LANES * (2 * r + a + 1)]
                t, off = divmod(LEVELS * g, LANES)
                if off:
                    piece = pltpu.roll(piece, off, 1)
                tiles[t] = piece if off == 0 else jnp.where(lane < off, tiles[t], piece)
                if off + LEVELS > LANES:
                    tiles[t + 1] = piece
            for t in range(TILES):
                wide_ref[pl.ds((2 * s + r) * TILES + t, WAYS, stride=PITCH), :] = tiles[t]
        return carry

    lax.fori_loop(0, SLOTS, synthesise, 0)
    for k in range(GRAD_ROWS):
        wide_ref[pl.ds(DATA_ROWS + k, WAYS, stride=PITCH), :] = jnp.broadcast_to(sums_ref[k : k + 1, :], (WAYS, LANES))
    pack_out(wide_ref, out_ref)


def spectral(wave_local, arrived, at, inv, synth):
    return pl.pallas_call(
        spectral_kernel,
        in_specs=[SMEM, VMEM, VMEM, ANY, ANY],
        out_specs=VMEM,
        out_shape=jax.ShapeDtypeStruct((WAYS, ROWS, LANES), jnp.bfloat16),
        scratch_shapes=[
            pltpu.VMEM((WAYS * PITCH, LANES), jnp.float32),
            pltpu.VMEM((NLAT, 4 * LANES), jnp.bfloat16),
            pltpu.VMEM((NDEG * BANK, LANES), jnp.float32),
            pltpu.VMEM((NDEG, LEVELS, LEVELS), jnp.bfloat16),
            pltpu.VMEM((SLOTS, NLAT, NDEG), jnp.bfloat16),
            pltpu.VMEM((24, LANES), jnp.float32),
            pltpu.SemaphoreType.DMA((2,)),
        ],
        compiler_params=params(58),
        name="spectral",
    )(wave_local, arrived, at, inv, synth)


def inverse_kernel(in_ref, table_ref, out_ref, g1, g2, g3, wide_ref, rows_ref, grad_ref):
    unpack_in(in_ref, wide_ref)
    for t in range(TILES):
        for c in range(2 * SLOTS):
            slab = wide_ref[pl.ds(TILES * c + t, WAYS, stride=PITCH), :]
            rows_ref[LANES * t : LANES * (t + 1), WAYS * c : WAYS * (c + 1)] = slab.T.astype(jnp.bfloat16)
    for i in range(SLOTS):
        out_ref[i] = mm(rows_ref[FEATURES * i : FEATURES * (i + 1), :], table_ref[...])
    for k in range(GRAD_ROWS):
        grad_ref[WAYS * k : WAYS * (k + 1), :] = wide_ref[pl.ds(DATA_ROWS + k, WAYS, stride=PITCH), :]
    scale = 1.0 / math.sqrt(NLAT * NLON)
    at = 0
    for g in (g1, g2, g3):
        rows = g.shape[0]
        for t in range(HIDDEN // LANES):
            g[:, LANES * t : LANES * (t + 1)] = grad_ref[at : at + rows, :] * scale
            at += rows


def inverse(arrived, table):
    return pl.pallas_call(
        inverse_kernel,
        in_specs=[VMEM] * 2,
        out_specs=[VMEM] * 4,
        out_shape=[
            jax.ShapeDtypeStruct((SLOTS, FEATURES, NLON), jnp.float32),
            jax.ShapeDtypeStruct((FEATURES, HIDDEN), jnp.float32),
            jax.ShapeDtypeStruct((HIDDEN, HIDDEN), jnp.float32),
            jax.ShapeDtypeStruct((FEATURES, HIDDEN), jnp.float32),
        ],
        scratch_shapes=[
            pltpu.VMEM((WAYS * PITCH, LANES), jnp.float32),
            pltpu.VMEM((WIDTH, NLON), jnp.bfloat16),
            pltpu.VMEM((GRAD_ROWS * WAYS, LANES), jnp.float32),
        ],
        compiler_params=params(48),
        name="inverse",
    )(arrived, table)


def swap(array, axis):
    return lax.all_to_all(array, axis, split_axis=0, concat_axis=0, tiled=True)


def on_device(x, c, wi, wm, wo, legendre, level_inverse, wave_order):
    x, c, wi, wm, wo = (pltpu.with_memory_space_constraint(a, pltpu.HBM) for a in (x, c, wi, wm, wo))
    grid, grad = columns(x, c, wi, wm, wo)
    grid, legendre, level_inverse, wave_order = lax.optimization_barrier((grid, legendre, level_inverse, wave_order))
    rows = swap(grid.reshape(8, LONB, WIDTH), "lev").reshape(NLON, WIDTH)
    wave_local = lax.dynamic_slice_in_dim(wave_order, lax.axis_index(EVERYWHERE) * SLOTS, SLOTS)
    table = wave_table(wave_order)
    at, synth = legendre_tables(wave_local, legendre)
    inv = level_inverse.transpose(2, 0, 1)
    arrived = swap(forward(rows, table, grad), EVERYWHERE)
    arrived = swap(spectral(wave_local, arrived, at, inv, synth), EVERYWHERE)
    out, g1, g2, g3 = inverse(arrived, table)
    return g1, g2, g3, out.transpose(1, 0, 2)


def solution(mesh):
    in_specs = (
        P(None, EVERYWHERE),
        P(None, EVERYWHERE),
        P(),
        P(),
        P(),
        P(EVERYWHERE, None, None),
        P(),
        P(),
    )
    out_specs = (P(), P(), P(), P(None, EVERYWHERE, None))
    return jax.shard_map(on_device, mesh=mesh, in_specs=in_specs, out_specs=out_specs, check_vma=False)
```

```python
import math

import jax
import jax.numpy as jnp
from jax import lax
from jax.experimental import pallas as pl
from jax.experimental.pallas import tpu as pltpu
from jax.sharding import PartitionSpec as P


NLAT = 640
NLON = 1280
LEVELS = 88
FEATURES = 176
HIDDEN = 384
NDEG = 640
HALF = NLAT // 2
SLOTS = 5
WAYS = 128
LONB = 160
LANES = 128
WIDTH = 896
TILES = WIDTH // LANES
ROWS = 72
GRAD_ROWS = 18
COLS = 6400
TILE = 256
STEPS = COLS // NLON
BANK = 25
INV_PARTS = 5
PITCH = 73
EVERYWHERE = ("lat", "lev")

VMEM = pl.BlockSpec(memory_space=pltpu.VMEM)
SMEM = pl.BlockSpec(memory_space=pltpu.SMEM)
ANY = pl.BlockSpec(memory_space=pl.ANY)


def mm(left, right):
    return jnp.dot(left, right, preferred_element_type=jnp.float32)


def mm_nt(left, right):
    return lax.dot_general(left, right, (((1,), (1,)), ((), ())), preferred_element_type=jnp.float32)


def mm_tn(left, right):
    return lax.dot_general(left, right, (((0,), (0,)), ((), ())), preferred_element_type=jnp.float32)


def params(mib):
    return pltpu.CompilerParams(vmem_limit_bytes=mib * 1024 * 1024)


def column_kernel(x_ref, c_ref, wi_ref, wm_ref, wo_ref, out_ref, grad_ref, wit, wmt, wot, wmh, h1_ref, h2_ref, d1_ref, d2_ref, s1_ref, grid_ref, g1, g2, g3):
    n = pl.program_id(0)

    @pl.when(n == 0)
    def _():
        half = jnp.bfloat16(0.5)
        wit[...] = wi_ref[...].T * half
        wmt[...] = wm_ref[...].T * half
        wot[...] = wo_ref[...].T * half
        wmh[...] = wm_ref[...] * half
        g1[...] = jnp.zeros_like(g1)
        g2[...] = jnp.zeros_like(g2)
        g3[...] = jnp.zeros_like(g3)
        grid_ref[SLOTS * FEATURES :, :] = jnp.zeros((WIDTH - SLOTS * FEATURES, NLON), jnp.bfloat16)

    band = pl.ds(pl.multiple_of(n * FEATURES, 16), FEATURES)
    tiles = [slice(TILE * t, TILE * (t + 1)) for t in range(NLON // TILE)]
    parts = [slice(384 * t, 384 * (t + 1)) for t in range(HIDDEN // 384)]
    for cols in tiles:
        for rows in parts:
            u = mm(wit[rows, :], x_ref[:, cols])
            tanh = jnp.tanh(u)
            p = 1.0 + tanh
            h1_ref[rows, cols] = (u * p).astype(jnp.bfloat16)
            s1_ref[rows, cols] = p * (1.0 + u * (1.0 - tanh))
    for cols in tiles:
        for rows in parts:
            u = mm(wmt[rows, :], h1_ref[:, cols])
            back = mm(wot[rows, :], c_ref[:, cols])
            tanh = jnp.tanh(u)
            p = 1.0 + tanh
            h2_ref[rows, cols] = (u * p).astype(jnp.bfloat16)
            d2_ref[rows, cols] = (back * (p * (1.0 + u * (1.0 - tanh)))).astype(jnp.bfloat16)
    for cols in tiles:
        for rows in parts:
            d1_ref[rows, cols] = (mm(wmh[rows, :], d2_ref[:, cols]) * s1_ref[rows, cols]).astype(jnp.bfloat16)
    for cols in tiles:
        grid_ref[band, cols] = mm(wi_ref[...], d1_ref[:, cols]).astype(jnp.bfloat16)
    g1[...] += mm_nt(x_ref[...], d1_ref[...])
    g2[...] += mm_nt(h1_ref[...], d2_ref[...])
    g3[...] += mm_nt(c_ref[...], h2_ref[...])

    @pl.when(n == STEPS - 1)
    def _():
        for t in range(TILES):
            out_ref[:, LANES * t : LANES * (t + 1)] = grid_ref[LANES * t : LANES * (t + 1), :].T
        at = 0
        for g in (g1, g2, g3):
            rows = g.shape[0]
            for t in range(HIDDEN // LANES):
                grad_ref[at : at + rows, :] = g[:, LANES * t : LANES * (t + 1)]
                at += rows
        grad_ref[at:, :] = jnp.zeros((GRAD_ROWS * WAYS - at, LANES), jnp.float32)


def columns(x, c, wi, wm, wo):
    block = pl.BlockSpec((FEATURES, NLON), lambda n: (0, n))
    kept = pltpu.VMEM((HIDDEN, NLON), jnp.bfloat16)
    return pl.pallas_call(
        column_kernel,
        grid=(STEPS,),
        in_specs=[block, block] + [pl.BlockSpec(w.shape, lambda n: (0, 0)) for w in (wi, wm, wo)],
        out_specs=[
            pl.BlockSpec((NLON, WIDTH), lambda n: (0, 0)),
            pl.BlockSpec((GRAD_ROWS * WAYS, LANES), lambda n: (0, 0)),
        ],
        out_shape=[
            jax.ShapeDtypeStruct((NLON, WIDTH), jnp.bfloat16),
            jax.ShapeDtypeStruct((GRAD_ROWS * WAYS, LANES), jnp.float32),
        ],
        scratch_shapes=[
            pltpu.VMEM((HIDDEN, FEATURES), jnp.bfloat16),
            pltpu.VMEM((HIDDEN, HIDDEN), jnp.bfloat16),
            pltpu.VMEM((HIDDEN, FEATURES), jnp.bfloat16),
            pltpu.VMEM((HIDDEN, HIDDEN), jnp.bfloat16),
            kept,
            kept,
            kept,
            kept,
            pltpu.VMEM((HIDDEN, NLON), jnp.float32),
            pltpu.VMEM((WIDTH, NLON), jnp.bfloat16),
            pltpu.VMEM((FEATURES, HIDDEN), jnp.float32),
            pltpu.VMEM((HIDDEN, HIDDEN), jnp.float32),
            pltpu.VMEM((FEATURES, HIDDEN), jnp.float32),
        ],
        compiler_params=params(48),
        name="columns",
    )(x, c, wi, wm, wo)


def wave_kernel(ca_ref, sa_ref, cb_ref, sb_ref, out_ref):
    for s in range(SLOTS):
        rows = slice(WAYS * s, WAYS * (s + 1))
        cb, sb = cb_ref[rows, :], sb_ref[rows, :]
        for a in range(NLON // LANES):
            ca, sa = ca_ref[rows, a : a + 1], sa_ref[rows, a : a + 1]
            cols = slice(LANES * a, LANES * (a + 1))
            out_ref[WAYS * 2 * s : WAYS * (2 * s + 1), cols] = (ca * cb - sa * sb).astype(jnp.bfloat16)
            out_ref[WAYS * (2 * s + 1) : WAYS * (2 * s + 2), cols] = (-(sa * cb + ca * sb)).astype(jnp.bfloat16)


def wave_table(wave_order):
    m = wave_order.reshape(WAYS, SLOTS).T.reshape(NLAT, 1)
    turn = 2.0 * math.pi / NLON
    fine = (m * jnp.arange(LANES, dtype=jnp.int32)[None, :] % NLON).astype(jnp.float32) * turn
    coarse = (m * (LANES * jnp.arange(NLON // LANES, dtype=jnp.int32))[None, :] % NLON).astype(jnp.float32) * turn
    scale = 1.0 / math.sqrt(NLON)
    return pl.pallas_call(
        wave_kernel,
        in_specs=[VMEM] * 4,
        out_specs=VMEM,
        out_shape=jax.ShapeDtypeStruct((NLON, NLON), jnp.bfloat16),
        compiler_params=params(32),
        name="waves",
    )(jnp.cos(coarse), jnp.sin(coarse), jnp.cos(fine) * scale, jnp.sin(fine) * scale)


def legendre_kernel(m_ref, leg_ref, at_ref, as_ref):
    m = m_ref[pl.program_id(0)]
    leg = leg_ref[0]
    row = lax.broadcasted_iota(jnp.int32, (HALF, NLAT), 0)
    col = lax.broadcasted_iota(jnp.int32, (HALF, NLAT), 1)
    lat = 40 * ((col & 127) >> 3) + 8 * (col >> 7) + (col & 7)
    pick = (jnp.where(lat < HALF, lat, NLAT - 1 - lat) == row).astype(jnp.bfloat16)
    full = mm_tn(leg, pick)
    deg = lax.broadcasted_iota(jnp.int32, (NDEG, NLAT), 0)
    col = lax.broadcasted_iota(jnp.int32, (NDEG, NLAT), 1)
    south = (col & 127) >= 64
    full = jnp.where(south & (((deg + m) & 1) == 1), -full, full)
    at_ref[0] = jnp.where(deg >= m, full, 0.0).astype(jnp.bfloat16)
    row = lax.broadcasted_iota(jnp.int32, (NLAT, HALF), 0)
    col = lax.broadcasted_iota(jnp.int32, (NLAT, HALF), 1)
    lat = 5 * (row & 127) + (row >> 7)
    pick = (jnp.where(lat < HALF, lat, NLAT - 1 - lat) == col).astype(jnp.bfloat16)
    full = mm(pick, leg)
    row = lax.broadcasted_iota(jnp.int32, (NLAT, NDEG), 0)
    deg = lax.broadcasted_iota(jnp.int32, (NLAT, NDEG), 1)
    south = (row & 127) >= 64
    full = jnp.where(south & (((deg + m) & 1) == 1), -full, full)
    as_ref[0] = jnp.where(deg >= m, full, 0.0).astype(jnp.bfloat16)


def legendre_tables(wave_local, legendre):
    block = pl.BlockSpec((1, NDEG, NLAT), lambda s, m: (s, 0, 0))
    table = jax.ShapeDtypeStruct((SLOTS, NDEG, NLAT), jnp.bfloat16)
    return pl.pallas_call(
        legendre_kernel,
        grid_spec=pltpu.PrefetchScalarGridSpec(
            num_scalar_prefetch=1,
            grid=(SLOTS,),
            in_specs=[pl.BlockSpec((1, HALF, NDEG), lambda s, m: (s, 0, 0))],
            out_specs=[block, block],
        ),
        out_shape=[table, table],
        compiler_params=params(40),
        name="legendre",
    )(wave_local, legendre)


def pack_out(wide_ref, out_ref):
    def body(p, carry):
        out_ref[p] = wide_ref[pl.ds(PITCH * p, ROWS), :].astype(jnp.bfloat16)
        return carry

    lax.fori_loop(0, WAYS, body, 0, unroll=4)


def unpack_in(in_ref, wide_ref):
    def body(p, carry):
        wide_ref[pl.ds(PITCH * p, ROWS), :] = in_ref[p].astype(jnp.float32)
        return carry

    lax.fori_loop(0, WAYS, body, 0, unroll=4)


def forward_kernel(x_ref, table_ref, out_ref, wide_ref):
    def body(k, carry):
        piece = mm(table_ref[pl.ds(pl.multiple_of(256 * k, 256), 256), :], x_ref[...])
        for h in range(2):
            for t in range(TILES):
                wide_ref[pl.ds((2 * k + h) * TILES + t, WAYS, stride=PITCH), :] = piece[
                    WAYS * h : WAYS * (h + 1), LANES * t : LANES * (t + 1)
                ]
        return carry

    lax.fori_loop(0, SLOTS, body, 0)
    pack_out(wide_ref, out_ref)


def forward(x, table):
    return pl.pallas_call(
        forward_kernel,
        in_specs=[VMEM] * 2,
        out_specs=VMEM,
        out_shape=jax.ShapeDtypeStruct((WAYS, ROWS, LANES), jnp.bfloat16),
        scratch_shapes=[pltpu.VMEM((WAYS * PITCH, LANES), jnp.float32)],
        compiler_params=params(24),
        name="forward",
    )(x, table)


def spectral_kernel(m_ref, in_ref, at_hbm, inv_hbm, as_hbm, out_ref, wide_ref, x_ref, bank_ref, at_ref, inv_ref, as_ref, sems):
    at_copy = pltpu.make_async_copy(at_hbm, at_ref, sems.at[0])
    inv_copies = []
    for k in range(INV_PARTS):
        part = pl.ds(k * (NDEG // INV_PARTS), NDEG // INV_PARTS)
        inv_copies.append(pltpu.make_async_copy(inv_hbm.at[part], inv_ref.at[part], sems.at[2 + k]))
    as_copy = pltpu.make_async_copy(as_hbm, as_ref, sems.at[1])
    at_copy.start()
    for copy in inv_copies:
        copy.start()
    as_copy.start()
    unpack_in(in_ref, wide_ref)
    lane = lax.broadcasted_iota(jnp.int32, (WAYS, LANES), 1)

    def analyse(s, carry):
        for r in range(2):
            tiles = [wide_ref[pl.ds((2 * s + r) * TILES + t, WAYS, stride=PITCH), :] for t in range(TILES)]
            for g in range(2 * SLOTS):
                t, off = divmod(LEVELS * g, LANES)
                piece = tiles[t]
                if off:
                    piece = pltpu.roll(piece, LANES - off, 1)
                    if off + LEVELS > LANES:
                        piece = jnp.where(lane < LANES - off, piece, pltpu.roll(tiles[t + 1], LANES - off, 1))
                i, a = divmod(g, 2)
                x_ref[WAYS * i : WAYS * (i + 1), LANES * (2 * r + a) : LANES * (2 * r + a + 1)] = piece.astype(jnp.bfloat16)
        y = mm(at_ref[s], x_ref[...])
        for j in range(4):
            bank_ref[pl.ds(4 * s + j, NDEG, stride=BANK), :] = y[:, LANES * j : LANES * (j + 1)]
        return carry

    at_copy.wait()
    lax.fori_loop(0, SLOTS, analyse, 0)

    def solve(k, carry):
        for u in range(16):
            deg = 16 * k + u
            rows = pl.ds(deg * BANK, 24)
            bank_ref[rows, :LEVELS] = mm(bank_ref[rows, :LEVELS].astype(jnp.bfloat16), inv_ref[deg])
        return carry

    steps = NDEG // 16 // INV_PARTS
    for k, copy in enumerate(inv_copies):
        copy.wait()
        lax.fori_loop(steps * k, steps * (k + 1), solve, 0)

    def synthesise(s, carry):
        z = jnp.concatenate(
            [bank_ref[pl.ds(4 * s + j, NDEG, stride=BANK), :].astype(jnp.bfloat16) for j in range(4)], axis=1
        )
        weight = jnp.where(m_ref[s] == 0, 1.0, 2.0)
        w = mm(as_ref[s], z) * weight
        for r in range(2):
            tiles = [None] * TILES
            for g in range(2 * SLOTS):
                i, a = divmod(g, 2)
                piece = w[WAYS * i : WAYS * (i + 1), LANES * (2 * r + a) : LANES * (2 * r + a + 1)]
                t, off = divmod(LEVELS * g, LANES)
                if off:
                    piece = pltpu.roll(piece, off, 1)
                tiles[t] = piece if off == 0 else jnp.where(lane < off, tiles[t], piece)
                if off + LEVELS > LANES:
                    tiles[t + 1] = piece
            for t in range(TILES):
                wide_ref[pl.ds((2 * s + r) * TILES + t, WAYS, stride=PITCH), :] = tiles[t]
        return carry

    as_copy.wait()
    lax.fori_loop(0, SLOTS, synthesise, 0)
    pack_out(wide_ref, out_ref)


def spectral(wave_local, arrived, at, inv, synth):
    return pl.pallas_call(
        spectral_kernel,
        in_specs=[SMEM, VMEM, ANY, ANY, ANY],
        out_specs=VMEM,
        out_shape=jax.ShapeDtypeStruct((WAYS, ROWS, LANES), jnp.bfloat16),
        scratch_shapes=[
            pltpu.VMEM((WAYS * PITCH, LANES), jnp.float32),
            pltpu.VMEM((NLAT, 4 * LANES), jnp.bfloat16),
            pltpu.VMEM((NDEG * BANK, LANES), jnp.float32),
            pltpu.VMEM((SLOTS, NDEG, NLAT), jnp.bfloat16),
            pltpu.VMEM((NDEG, LEVELS, LEVELS), jnp.bfloat16),
            pltpu.VMEM((SLOTS, NLAT, NDEG), jnp.bfloat16),
            pltpu.SemaphoreType.DMA((2 + INV_PARTS,)),
        ],
        compiler_params=params(46),
        name="spectral",
    )(wave_local, arrived, at, inv, synth)


def inverse_kernel(in_ref, table_ref, out_ref, wide_ref, rows_ref):
    unpack_in(in_ref, wide_ref)
    for t in range(TILES):
        for c in range(2 * SLOTS):
            slab = wide_ref[pl.ds(TILES * c + t, WAYS, stride=PITCH), :]
            rows_ref[LANES * t : LANES * (t + 1), WAYS * c : WAYS * (c + 1)] = slab.T.astype(jnp.bfloat16)
    for i in range(SLOTS):
        out_ref[i] = mm(rows_ref[FEATURES * i : FEATURES * (i + 1), :], table_ref[...])


def inverse(arrived, table):
    return pl.pallas_call(
        inverse_kernel,
        in_specs=[VMEM] * 2,
        out_specs=VMEM,
        out_shape=jax.ShapeDtypeStruct((SLOTS, FEATURES, NLON), jnp.float32),
        scratch_shapes=[
            pltpu.VMEM((WAYS * PITCH, LANES), jnp.float32),
            pltpu.VMEM((WIDTH, NLON), jnp.bfloat16),
        ],
        compiler_params=params(28),
        name="inverse",
    )(arrived, table)


def unstack_kernel(in_ref, g1, g2, g3):
    scale = 1.0 / math.sqrt(NLAT * NLON)
    at = 0
    for g in (g1, g2, g3):
        rows = g.shape[0]
        for t in range(HIDDEN // LANES):
            g[:, LANES * t : LANES * (t + 1)] = in_ref[at : at + rows, :].astype(jnp.float32) * scale
            at += rows


def unstack(grad):
    return pl.pallas_call(
        unstack_kernel,
        in_specs=[VMEM],
        out_specs=[VMEM] * 3,
        out_shape=[jax.ShapeDtypeStruct((r, HIDDEN), jnp.float32) for r in (FEATURES, HIDDEN, FEATURES)],
        compiler_params=params(8),
        name="unstack",
    )(grad)


STAGES = (("lev", 1), ("lat", 1), ("lat", 4), ("lat", 2), ("lat", 8), ("lev", 2), ("lev", 4))
EARLY = 4


def across(array, axis, bit):
    size = lax.axis_size(axis)
    return lax.ppermute(array, axis, [(i, i ^ bit) for i in range(size)])


def upper(axis, bit):
    return (lax.axis_index(axis) & bit) != 0


def halve(total, axis, bit):
    half = total.shape[0] // 2
    low, high = total[:half], total[half:]
    mine = upper(axis, bit)
    sent = jnp.where(mine, low, high).astype(jnp.bfloat16)
    return jnp.where(mine, high, low) + across(sent, axis, bit).astype(jnp.float32)


def double(part, axis, bit):
    other = across(part, axis, bit)
    mine = upper(axis, bit)
    return jnp.concatenate([jnp.where(mine, other, part), jnp.where(mine, part, other)])


def swap(array, axis):
    return lax.all_to_all(array, axis, split_axis=0, concat_axis=0, tiled=True)


def program(x, c, wi, wm, wo, legendre, level_inverse, wave_order):
    x, c, wi, wm, wo = (pltpu.with_memory_space_constraint(a, pltpu.HBM) for a in (x, c, wi, wm, wo))
    grid, grad = columns(x, c, wi, wm, wo)
    grid, legendre, level_inverse, wave_order = lax.optimization_barrier((grid, legendre, level_inverse, wave_order))
    rows = swap(grid.reshape(8, LONB, WIDTH), "lev")
    rows = rows.reshape(NLON, WIDTH)
    wave_local = lax.dynamic_slice_in_dim(wave_order, lax.axis_index(EVERYWHERE) * SLOTS, SLOTS)
    table = wave_table(wave_order)
    for axis, bit in STAGES[:EARLY]:
        grad = halve(grad, axis, bit)
    rows, table, grad = lax.optimization_barrier((rows, table, grad))
    at, synth = legendre_tables(wave_local, legendre)
    inv = level_inverse.transpose(2, 0, 1)
    arrived = swap(forward(rows, table), EVERYWHERE)
    zonal = spectral(wave_local, arrived, at, inv, synth)
    zonal, grad = lax.optimization_barrier((zonal, grad))
    for axis, bit in STAGES[EARLY:]:
        grad = halve(grad, axis, bit)
    grad = grad.astype(jnp.bfloat16)
    for axis, bit in STAGES[::-1]:
        grad = double(grad, axis, bit)
    g1, g2, g3 = unstack(grad)
    arrived = swap(zonal, EVERYWHERE)
    out = inverse(arrived, table)
    return g1, g2, g3, out.transpose(1, 0, 2)


def solution(mesh):
    in_specs = (
        P(None, EVERYWHERE),
        P(None, EVERYWHERE),
        P(),
        P(),
        P(),
        P(EVERYWHERE, None, None),
        P(),
        P(),
    )
    out_specs = (P(), P(), P(), P(None, EVERYWHERE, None))
    return jax.shard_map(program, mesh=mesh, in_specs=in_specs, out_specs=out_specs, check_vma=False)
```

```python
import math

import jax
import jax.numpy as jnp
from jax import lax
from jax.experimental import pallas as pl
from jax.experimental.pallas import tpu as pltpu
from jax.sharding import PartitionSpec as P


NLAT = 640
NLON = 1280
LEVELS = 88
FEATURES = 176
HIDDEN = 384
NDEG = 640
HALF = NLAT // 2
SLOTS = 5
WAYS = 128
LONB = 160
LANES = 128
WIDTH = 896
TILES = WIDTH // LANES
DATA_ROWS = 2 * SLOTS * TILES
ROWS = 72
LATE_ROWS = 88
GRAD_ROWS = 18
BLOCKS = 32
BLOCK_ROWS = 72
COLS = 6400
TILE = 256
STEPS = COLS // NLON
BANK = 25
INV_PARTS = 5
PITCH = 73
LATE_PITCH = 89
EVERYWHERE = ("lat", "lev")

VMEM = pl.BlockSpec(memory_space=pltpu.VMEM)
SMEM = pl.BlockSpec(memory_space=pltpu.SMEM)
ANY = pl.BlockSpec(memory_space=pl.ANY)
HBM = pl.BlockSpec(memory_space=pltpu.HBM)
GROUPS = 8
GROUP = WAYS // GROUPS


def mm(left, right):
    return jnp.dot(left, right, preferred_element_type=jnp.float32)


def mm_nt(left, right):
    return lax.dot_general(left, right, (((1,), (1,)), ((), ())), preferred_element_type=jnp.float32)


def mm_tn(left, right):
    return lax.dot_general(left, right, (((0,), (0,)), ((), ())), preferred_element_type=jnp.float32)


def params(mib):
    return pltpu.CompilerParams(vmem_limit_bytes=mib * 1024 * 1024)


def column_kernel(x_ref, c_ref, wi_ref, wm_ref, wo_ref, out_hbm, grad_ref, wit, wmt, wot, wmh, h1_ref, h2_ref, d1_ref, d2_ref, s1_ref, grid_ref, g1, g2, g3, out_ref, sems):
    n = pl.program_id(0)

    @pl.when(n == 0)
    def _():
        half = jnp.bfloat16(0.5)
        wit[...] = wi_ref[...].T * half
        wmt[...] = wm_ref[...].T * half
        wot[...] = wo_ref[...].T * half
        wmh[...] = wm_ref[...] * half
        g1[...] = jnp.zeros_like(g1)
        g2[...] = jnp.zeros_like(g2)
        g3[...] = jnp.zeros_like(g3)
        grid_ref[SLOTS * FEATURES :, :] = jnp.zeros((WIDTH - SLOTS * FEATURES, NLON), jnp.bfloat16)

    band = pl.ds(pl.multiple_of(n * FEATURES, 16), FEATURES)
    tiles = [slice(TILE * t, TILE * (t + 1)) for t in range(NLON // TILE)]
    parts = [slice(384 * t, 384 * (t + 1)) for t in range(HIDDEN // 384)]
    for cols in tiles:
        for rows in parts:
            u = mm(wit[rows, :], x_ref[:, cols])
            tanh = jnp.tanh(u)
            p = 1.0 + tanh
            h1_ref[rows, cols] = (u * p).astype(jnp.bfloat16)
            s1_ref[rows, cols] = p * (1.0 + u * (1.0 - tanh))
    for cols in tiles:
        for rows in parts:
            u = mm(wmt[rows, :], h1_ref[:, cols])
            back = mm(wot[rows, :], c_ref[:, cols])
            tanh = jnp.tanh(u)
            p = 1.0 + tanh
            h2_ref[rows, cols] = (u * p).astype(jnp.bfloat16)
            d2_ref[rows, cols] = (back * (p * (1.0 + u * (1.0 - tanh)))).astype(jnp.bfloat16)
    for cols in tiles:
        for rows in parts:
            d1_ref[rows, cols] = (mm(wmh[rows, :], d2_ref[:, cols]) * s1_ref[rows, cols]).astype(jnp.bfloat16)
    for cols in tiles:
        grid_ref[band, cols] = mm(wi_ref[...], d1_ref[:, cols]).astype(jnp.bfloat16)
    g1[...] += mm_nt(x_ref[...], d1_ref[...])
    g2[...] += mm_nt(h1_ref[...], d2_ref[...])
    g3[...] += mm_nt(c_ref[...], h2_ref[...])

    @pl.when(n == STEPS - 1)
    def _():
        copies = [
            pltpu.make_async_copy(out_ref.at[:, pl.ds(LANES * t, LANES)], out_hbm.at[:, pl.ds(LANES * t, LANES)], sems.at[t])
            for t in range(TILES)
        ]
        for t in range(TILES):
            out_ref[:, LANES * t : LANES * (t + 1)] = grid_ref[LANES * t : LANES * (t + 1), :].T
            copies[t].start()
        for copy in copies:
            copy.wait()
        at = 0
        for g in (g1, g2, g3):
            rows = g.shape[0]
            for t in range(HIDDEN // LANES):
                grad_ref[at : at + rows, :] = g[:, LANES * t : LANES * (t + 1)]
                at += rows
        grad_ref[at:, :] = jnp.zeros((GRAD_ROWS * WAYS - at, LANES), jnp.float32)


def columns(x, c, wi, wm, wo):
    block = pl.BlockSpec((FEATURES, NLON), lambda n: (0, n))
    kept = pltpu.VMEM((HIDDEN, NLON), jnp.bfloat16)
    return pl.pallas_call(
        column_kernel,
        grid=(STEPS,),
        in_specs=[block, block] + [pl.BlockSpec(w.shape, lambda n: (0, 0)) for w in (wi, wm, wo)],
        out_specs=[
            HBM,
            pl.BlockSpec((GRAD_ROWS * WAYS, LANES), lambda n: (0, 0)),
        ],
        out_shape=[
            jax.ShapeDtypeStruct((NLON, WIDTH), jnp.bfloat16),
            jax.ShapeDtypeStruct((GRAD_ROWS * WAYS, LANES), jnp.float32),
        ],
        scratch_shapes=[
            pltpu.VMEM((HIDDEN, FEATURES), jnp.bfloat16),
            pltpu.VMEM((HIDDEN, HIDDEN), jnp.bfloat16),
            pltpu.VMEM((HIDDEN, FEATURES), jnp.bfloat16),
            pltpu.VMEM((HIDDEN, HIDDEN), jnp.bfloat16),
            kept,
            kept,
            kept,
            kept,
            pltpu.VMEM((HIDDEN, NLON), jnp.float32),
            pltpu.VMEM((WIDTH, NLON), jnp.bfloat16),
            pltpu.VMEM((FEATURES, HIDDEN), jnp.float32),
            pltpu.VMEM((HIDDEN, HIDDEN), jnp.float32),
            pltpu.VMEM((FEATURES, HIDDEN), jnp.float32),
            pltpu.VMEM((NLON, WIDTH), jnp.bfloat16),
            pltpu.SemaphoreType.DMA((TILES,)),
        ],
        compiler_params=params(60),
        name="columns",
    )(x, c, wi, wm, wo)


def wave_kernel(ca_ref, sa_ref, cb_ref, sb_ref, out_ref):
    for s in range(SLOTS):
        rows = slice(WAYS * s, WAYS * (s + 1))
        cb, sb = cb_ref[rows, :], sb_ref[rows, :]
        for a in range(NLON // LANES):
            ca, sa = ca_ref[rows, a : a + 1], sa_ref[rows, a : a + 1]
            cols = slice(LANES * a, LANES * (a + 1))
            out_ref[WAYS * 2 * s : WAYS * (2 * s + 1), cols] = (ca * cb - sa * sb).astype(jnp.bfloat16)
            out_ref[WAYS * (2 * s + 1) : WAYS * (2 * s + 2), cols] = (-(sa * cb + ca * sb)).astype(jnp.bfloat16)


def wave_table(wave_order):
    m = wave_order.reshape(WAYS, SLOTS).T.reshape(NLAT, 1)
    turn = 2.0 * math.pi / NLON
    fine = (m * jnp.arange(LANES, dtype=jnp.int32)[None, :] % NLON).astype(jnp.float32) * turn
    coarse = (m * (LANES * jnp.arange(NLON // LANES, dtype=jnp.int32))[None, :] % NLON).astype(jnp.float32) * turn
    scale = 1.0 / math.sqrt(NLON)
    return pl.pallas_call(
        wave_kernel,
        in_specs=[VMEM] * 4,
        out_specs=VMEM,
        out_shape=jax.ShapeDtypeStruct((NLON, NLON), jnp.bfloat16),
        compiler_params=params(32),
        name="waves",
    )(jnp.cos(coarse), jnp.sin(coarse), jnp.cos(fine) * scale, jnp.sin(fine) * scale)


def legendre_kernel(m_ref, leg_ref, at_ref, as_ref):
    m = m_ref[pl.program_id(0)]
    leg = leg_ref[0]
    row = lax.broadcasted_iota(jnp.int32, (HALF, NLAT), 0)
    col = lax.broadcasted_iota(jnp.int32, (HALF, NLAT), 1)
    lat = 40 * ((col & 127) >> 3) + 8 * (col >> 7) + (col & 7)
    pick = (jnp.where(lat < HALF, lat, NLAT - 1 - lat) == row).astype(jnp.bfloat16)
    full = mm_tn(leg, pick)
    deg = lax.broadcasted_iota(jnp.int32, (NDEG, NLAT), 0)
    col = lax.broadcasted_iota(jnp.int32, (NDEG, NLAT), 1)
    south = (col & 127) >= 64
    full = jnp.where(south & (((deg + m) & 1) == 1), -full, full)
    at_ref[0] = jnp.where(deg >= m, full, 0.0).astype(jnp.bfloat16)
    row = lax.broadcasted_iota(jnp.int32, (NLAT, HALF), 0)
    col = lax.broadcasted_iota(jnp.int32, (NLAT, HALF), 1)
    lat = 5 * (row & 127) + (row >> 7)
    pick = (jnp.where(lat < HALF, lat, NLAT - 1 - lat) == col).astype(jnp.bfloat16)
    full = mm(pick, leg)
    row = lax.broadcasted_iota(jnp.int32, (NLAT, NDEG), 0)
    deg = lax.broadcasted_iota(jnp.int32, (NLAT, NDEG), 1)
    south = (row & 127) >= 64
    full = jnp.where(south & (((deg + m) & 1) == 1), -full, full)
    as_ref[0] = jnp.where(deg >= m, full, 0.0).astype(jnp.bfloat16)


def legendre_tables(wave_local, legendre):
    block = pl.BlockSpec((1, NDEG, NLAT), lambda s, m: (s, 0, 0))
    table = jax.ShapeDtypeStruct((SLOTS, NDEG, NLAT), jnp.bfloat16)
    return pl.pallas_call(
        legendre_kernel,
        grid_spec=pltpu.PrefetchScalarGridSpec(
            num_scalar_prefetch=1,
            grid=(SLOTS,),
            in_specs=[pl.BlockSpec((1, HALF, NDEG), lambda s, m: (s, 0, 0))],
            out_specs=[block, block],
        ),
        out_shape=[table, table],
        compiler_params=params(60),
        name="legendre",
    )(wave_local, legendre)


def group_copies(src, dst, sems):
    return [pltpu.make_async_copy(src.at[pl.ds(GROUP * k, GROUP)], dst.at[pl.ds(GROUP * k, GROUP)], sems.at[k]) for k in range(GROUPS)]


def pack_out(wide_ref, chunk_ref, out_hbm, sems, pitch):
    rows = chunk_ref.shape[1]

    def body(p, carry):
        chunk_ref[p] = wide_ref[pl.ds(pitch * p, rows), :].astype(jnp.bfloat16)
        return carry

    copies = group_copies(chunk_ref, out_hbm, sems)
    for k, copy in enumerate(copies):
        lax.fori_loop(GROUP * k, GROUP * (k + 1), body, 0, unroll=4)
        copy.start()
    for copy in copies:
        copy.wait()


def unpack_in(in_hbm, chunk_ref, wide_ref, sems, pitch, then=()):
    rows = chunk_ref.shape[1]

    def body(p, carry):
        wide_ref[pl.ds(pitch * p, rows), :] = chunk_ref[p].astype(jnp.float32)
        return carry

    copies = group_copies(in_hbm, chunk_ref, sems)
    for copy in (*copies, *then):
        copy.start()
    for k, copy in enumerate(copies):
        copy.wait()
        lax.fori_loop(GROUP * k, GROUP * (k + 1), body, 0, unroll=4)


CHUNKS = pltpu.VMEM((WAYS, ROWS, LANES), jnp.bfloat16)
LATE_CHUNKS = pltpu.VMEM((WAYS, LATE_ROWS, LANES), jnp.bfloat16)
GROUP_SEMS = pltpu.SemaphoreType.DMA((GROUPS,))


def forward_kernel(x_ref, table_ref, grad_ref, out_hbm, wide_ref, chunk_ref, sems):
    def body(k, carry):
        piece = mm(table_ref[pl.ds(pl.multiple_of(256 * k, 256), 256), :], x_ref[...])
        for h in range(2):
            for t in range(TILES):
                wide_ref[pl.ds((2 * k + h) * TILES + t, WAYS, stride=PITCH), :] = piece[
                    WAYS * h : WAYS * (h + 1), LANES * t : LANES * (t + 1)
                ]
        return carry

    lax.fori_loop(0, SLOTS, body, 0)
    for k in range(2):
        wide_ref[pl.ds(DATA_ROWS + k, WAYS, stride=PITCH), :] = jnp.zeros((WAYS, LANES), jnp.float32)
    wide_ref[pl.ds(DATA_ROWS, WAYS, stride=PITCH), :BLOCK_ROWS] = grad_ref[...].T
    pack_out(wide_ref, chunk_ref, out_hbm, sems, PITCH)


def forward(x, table, grad):
    return pl.pallas_call(
        forward_kernel,
        in_specs=[VMEM] * 3,
        out_specs=HBM,
        out_shape=jax.ShapeDtypeStruct((WAYS, ROWS, LANES), jnp.bfloat16),
        scratch_shapes=[pltpu.VMEM((WAYS * PITCH, LANES), jnp.float32), CHUNKS, GROUP_SEMS],
        compiler_params=params(24),
        name="forward",
    )(x, table, grad)


def sum_blocks(wide_ref, sums_ref):
    slab = wide_ref[pl.ds(DATA_ROWS, WAYS, stride=PITCH), :].astype(jnp.bfloat16)
    block = lax.broadcasted_iota(jnp.int32, (BLOCKS, WAYS), 0)
    source = lax.broadcasted_iota(jnp.int32, (BLOCKS, WAYS), 1)
    lat = source >> 3
    owner = ((source & 1) << 4) | ((lat & 1) << 3) | (((lat >> 2) & 1) << 2) | (((lat >> 1) & 1) << 1) | (lat >> 3)
    sums = mm((owner == block).astype(jnp.bfloat16), slab)
    half = BLOCKS // 2
    lane = lax.broadcasted_iota(jnp.int32, (half, LANES), 1)
    sums_ref[:half, :] = jnp.where(lane < 64, sums[:half], pltpu.roll(sums[half:], 64, 1))
    row = lax.broadcasted_iota(jnp.int32, (LANES, LANES), 0)
    col = lax.broadcasted_iota(jnp.int32, (LANES, LANES), 1)
    rest = mm(sums.astype(jnp.bfloat16), (row == 64 + (col & 7)).astype(jnp.bfloat16))
    keep = (lane >> 3) == lax.broadcasted_iota(jnp.int32, (half, LANES), 0)
    for h in range(2):
        part = jnp.where(keep, rest[half * h : half * (h + 1)], 0.0)
        sums_ref[half + h : half + h + 1, :] = jnp.sum(part, axis=0, keepdims=True)


def spectral_kernel(
    m_ref, in_hbm, at_hbm, inv_hbm, as_hbm, out_hbm, wide_ref, chunk_ref, late_ref, x_ref, bank_ref, at_ref, inv_ref, as_ref, sums_ref, sems, group_sems
):
    at_copy = pltpu.make_async_copy(at_hbm, at_ref, sems.at[0])
    inv_copies = []
    for k in range(INV_PARTS):
        part = pl.ds(k * (NDEG // INV_PARTS), NDEG // INV_PARTS)
        inv_copies.append(pltpu.make_async_copy(inv_hbm.at[part], inv_ref.at[part], sems.at[2 + k]))
    as_copy = pltpu.make_async_copy(as_hbm, as_ref, sems.at[1])
    unpack_in(in_hbm, chunk_ref, wide_ref, group_sems, PITCH, [at_copy, *inv_copies, as_copy])
    sum_blocks(wide_ref, sums_ref)
    lane = lax.broadcasted_iota(jnp.int32, (WAYS, LANES), 1)

    def analyse(s, carry):
        for r in range(2):
            tiles = [wide_ref[pl.ds((2 * s + r) * TILES + t, WAYS, stride=PITCH), :] for t in range(TILES)]
            for g in range(2 * SLOTS):
                t, off = divmod(LEVELS * g, LANES)
                piece = tiles[t]
                if off:
                    piece = pltpu.roll(piece, LANES - off, 1)
                    if off + LEVELS > LANES:
                        piece = jnp.where(lane < LANES - off, piece, pltpu.roll(tiles[t + 1], LANES - off, 1))
                i, a = divmod(g, 2)
                x_ref[WAYS * i : WAYS * (i + 1), LANES * (2 * r + a) : LANES * (2 * r + a + 1)] = piece.astype(jnp.bfloat16)
        y = mm(at_ref[s], x_ref[...])
        for j in range(4):
            bank_ref[pl.ds(4 * s + j, NDEG, stride=BANK), :] = y[:, LANES * j : LANES * (j + 1)]
        return carry

    at_copy.wait()
    lax.fori_loop(0, SLOTS, analyse, 0)

    def solve(k, carry):
        for u in range(16):
            deg = 16 * k + u
            rows = pl.ds(deg * BANK, 24)
            bank_ref[rows, :LEVELS] = mm(bank_ref[rows, :LEVELS].astype(jnp.bfloat16), inv_ref[deg])
        return carry

    steps = NDEG // 16 // INV_PARTS
    for k, copy in enumerate(inv_copies):
        copy.wait()
        lax.fori_loop(steps * k, steps * (k + 1), solve, 0)

    def synthesise(s, carry):
        z = jnp.concatenate(
            [bank_ref[pl.ds(4 * s + j, NDEG, stride=BANK), :].astype(jnp.bfloat16) for j in range(4)], axis=1
        )
        weight = jnp.where(m_ref[s] == 0, 1.0, 2.0)
        w = mm(as_ref[s], z) * weight
        for r in range(2):
            tiles = [None] * TILES
            for g in range(2 * SLOTS):
                i, a = divmod(g, 2)
                piece = w[WAYS * i : WAYS * (i + 1), LANES * (2 * r + a) : LANES * (2 * r + a + 1)]
                t, off = divmod(LEVELS * g, LANES)
                if off:
                    piece = pltpu.roll(piece, off, 1)
                tiles[t] = piece if off == 0 else jnp.where(lane < off, tiles[t], piece)
                if off + LEVELS > LANES:
                    tiles[t + 1] = piece
            for t in range(TILES):
                wide_ref[pl.ds((2 * s + r) * TILES + t, WAYS, stride=LATE_PITCH), :] = tiles[t]
        return carry

    as_copy.wait()
    lax.fori_loop(0, SLOTS, synthesise, 0)
    for k in range(GRAD_ROWS):
        row = jnp.broadcast_to(sums_ref[k : k + 1, :], (WAYS, LANES))
        wide_ref[pl.ds(DATA_ROWS + k, WAYS, stride=LATE_PITCH), :] = row
    pack_out(wide_ref, late_ref, out_hbm, group_sems, LATE_PITCH)


def spectral(wave_local, arrived, at, inv, synth):
    return pl.pallas_call(
        spectral_kernel,
        in_specs=[SMEM, ANY, ANY, ANY, ANY],
        out_specs=HBM,
        out_shape=jax.ShapeDtypeStruct((WAYS, LATE_ROWS, LANES), jnp.bfloat16),
        scratch_shapes=[
            pltpu.VMEM((WAYS * LATE_PITCH, LANES), jnp.float32),
            CHUNKS,
            LATE_CHUNKS,
            pltpu.VMEM((NLAT, 4 * LANES), jnp.bfloat16),
            pltpu.VMEM((NDEG * BANK, LANES), jnp.float32),
            pltpu.VMEM((SLOTS, NDEG, NLAT), jnp.bfloat16),
            pltpu.VMEM((NDEG, LEVELS, LEVELS), jnp.bfloat16),
            pltpu.VMEM((SLOTS, NLAT, NDEG), jnp.bfloat16),
            pltpu.VMEM((24, LANES), jnp.float32),
            pltpu.SemaphoreType.DMA((2 + INV_PARTS,)),
            GROUP_SEMS,
        ],
        compiler_params=params(60),
        name="spectral",
    )(wave_local, arrived, at, inv, synth)


def inverse_kernel(in_hbm, table_ref, out_hbm, g1, g2, g3, wide_ref, chunk_ref, rows_ref, out_ref, grad_ref, group_sems, sems):
    unpack_in(in_hbm, chunk_ref, wide_ref, group_sems, LATE_PITCH)
    for t in range(TILES):
        for c in range(2 * SLOTS):
            slab = wide_ref[pl.ds(TILES * c + t, WAYS, stride=LATE_PITCH), :]
            rows_ref[LANES * t : LANES * (t + 1), WAYS * c : WAYS * (c + 1)] = slab.T.astype(jnp.bfloat16)
    copies = []
    for i in range(SLOTS):
        out_ref[i] = mm(rows_ref[FEATURES * i : FEATURES * (i + 1), :], table_ref[...])
        copies.append(pltpu.make_async_copy(out_ref.at[i], out_hbm.at[i], sems.at[i]))
        copies[i].start()
    half = BLOCKS // 2
    for k in range(half):
        both = wide_ref[pl.ds(DATA_ROWS + k, WAYS, stride=LATE_PITCH), :].T
        for h in range(2):
            at = BLOCK_ROWS * (k + half * h)
            grad_ref[at : at + 64, :] = both[64 * h : 64 * (h + 1), :]
    for h in range(2):
        rest = wide_ref[pl.ds(DATA_ROWS + half + h, WAYS, stride=LATE_PITCH), :].T
        for k in range(half):
            at = BLOCK_ROWS * (k + half * h) + 64
            grad_ref[at : at + 8, :] = rest[8 * k : 8 * (k + 1), :]
    scale = 1.0 / math.sqrt(NLAT * NLON)
    at = 0
    for g in (g1, g2, g3):
        rows = g.shape[0]
        for t in range(HIDDEN // LANES):
            g[:, LANES * t : LANES * (t + 1)] = grad_ref[at : at + rows, :] * scale
            at += rows
    for copy in copies:
        copy.wait()


def inverse(arrived, table):
    return pl.pallas_call(
        inverse_kernel,
        in_specs=[ANY, VMEM],
        out_specs=[HBM, VMEM, VMEM, VMEM],
        out_shape=[jax.ShapeDtypeStruct((SLOTS, FEATURES, NLON), jnp.float32)]
        + [jax.ShapeDtypeStruct((r, HIDDEN), jnp.float32) for r in (FEATURES, HIDDEN, FEATURES)],
        scratch_shapes=[
            pltpu.VMEM((WAYS * LATE_PITCH, LANES), jnp.float32),
            LATE_CHUNKS,
            pltpu.VMEM((WIDTH, NLON), jnp.bfloat16),
            pltpu.VMEM((SLOTS, FEATURES, NLON), jnp.float32),
            pltpu.VMEM((GRAD_ROWS * WAYS, LANES), jnp.float32),
            GROUP_SEMS,
            pltpu.SemaphoreType.DMA((SLOTS,)),
        ],
        compiler_params=params(28),
        name="inverse",
    )(arrived, table)


STAGES = (("lev", 1), ("lat", 1), ("lat", 4), ("lat", 2), ("lat", 8))


def across(array, axis, bit):
    size = lax.axis_size(axis)
    return lax.ppermute(array, axis, [(i, i ^ bit) for i in range(size)])


def upper(axis, bit):
    return (lax.axis_index(axis) & bit) != 0


def halve(total, axis, bit):
    half = total.shape[0] // 2
    low, high = total[:half], total[half:]
    mine = upper(axis, bit)
    sent = jnp.where(mine, low, high).astype(jnp.bfloat16)
    return jnp.where(mine, high, low) + across(sent, axis, bit).astype(jnp.float32)


def in_hbm(array):
    return pltpu.with_memory_space_constraint(array, pltpu.HBM)


def swap(array, axis):
    return lax.all_to_all(array, axis, split_axis=0, concat_axis=0, tiled=True)


def program(x, c, wi, wm, wo, legendre, level_inverse, wave_order):
    grid, grad = columns(*map(in_hbm, (x, c, wi, wm, wo)))
    grid, legendre, level_inverse, wave_order = lax.optimization_barrier((grid, legendre, level_inverse, wave_order))
    rows = swap(grid.reshape(8, LONB, WIDTH), "lev")
    rows = rows.reshape(NLON, WIDTH)
    wave_local = lax.dynamic_slice_in_dim(wave_order, lax.axis_index(EVERYWHERE) * SLOTS, SLOTS)
    table = wave_table(wave_order)
    for axis, bit in STAGES:
        grad = halve(grad, axis, bit)
    rows, table, grad = lax.optimization_barrier((rows, table, grad))
    at, synth = legendre_tables(wave_local, legendre)
    inv = level_inverse.transpose(2, 0, 1)
    arrived = swap(forward(rows, table, grad), EVERYWHERE)
    zonal = spectral(wave_local, arrived, at, inv, synth)
    out, g1, g2, g3 = inverse(swap(zonal, EVERYWHERE), table)
    return g1, g2, g3, out.transpose(1, 0, 2)


def solution(mesh):
    in_specs = (
        P(None, EVERYWHERE),
        P(None, EVERYWHERE),
        P(),
        P(),
        P(),
        P(EVERYWHERE, None, None),
        P(),
        P(),
    )
    out_specs = (P(), P(), P(), P(None, EVERYWHERE, None))
    return jax.shard_map(program, mesh=mesh, in_specs=in_specs, out_specs=out_specs, check_vma=False)
```

```python
import math

import jax
import jax.numpy as jnp
from jax import lax
from jax.experimental import pallas as pl
from jax.experimental.pallas import tpu as pltpu
from jax.sharding import PartitionSpec as P


NLAT = 640
NLON = 1280
LEVELS = 88
FEATURES = 176
HIDDEN = 384
NDEG = 640
HALF = NLAT // 2
SLOTS = 5
WAYS = 128
LONB = 160
LANES = 128
WIDTH = 896
TILES = WIDTH // LANES
DATA_ROWS = 2 * SLOTS * TILES
ROWS = 72
LATE_ROWS = 88
GRAD_ROWS = 18
BLOCKS = 32
BLOCK_ROWS = 72
COLS = 6400
TILE = 256
STEPS = COLS // NLON
BANK = 25
INV_PARTS = 5
AHEAD = 3
PITCH = 73
LATE_PITCH = 89
EVERYWHERE = ("lat", "lev")

VMEM = pl.BlockSpec(memory_space=pltpu.VMEM)
SMEM = pl.BlockSpec(memory_space=pltpu.SMEM)
ANY = pl.BlockSpec(memory_space=pl.ANY)
HBM = pl.BlockSpec(memory_space=pltpu.HBM)
GROUPS = 8
GROUP = WAYS // GROUPS


def mm(left, right):
    return jnp.dot(left, right, preferred_element_type=jnp.float32)


def mm_nt(left, right):
    return lax.dot_general(left, right, (((1,), (1,)), ((), ())), preferred_element_type=jnp.float32)


def mm_tn(left, right):
    return lax.dot_general(left, right, (((0,), (0,)), ((), ())), preferred_element_type=jnp.float32)


def params(mib):
    return pltpu.CompilerParams(vmem_limit_bytes=mib * 1024 * 1024)


def column_kernel(x_ref, c_ref, wi_ref, wm_ref, wo_ref, out_hbm, grad_ref, wit, wmt, wot, wmh, h1_ref, h2_ref, d1_ref, d2_ref, s1_ref, grid_ref, g1, g2, g3, out_ref, sems):
    n = pl.program_id(0)

    @pl.when(n == 0)
    def _():
        half = jnp.bfloat16(0.5)
        wit[...] = wi_ref[...].T * half
        wmt[...] = wm_ref[...].T * half
        wot[...] = wo_ref[...].T * half
        wmh[...] = wm_ref[...] * half
        g1[...] = jnp.zeros_like(g1)
        g2[...] = jnp.zeros_like(g2)
        g3[...] = jnp.zeros_like(g3)
        grid_ref[SLOTS * FEATURES :, :] = jnp.zeros((WIDTH - SLOTS * FEATURES, NLON), jnp.bfloat16)

    band = pl.ds(pl.multiple_of(n * FEATURES, 16), FEATURES)
    tiles = [slice(TILE * t, TILE * (t + 1)) for t in range(NLON // TILE)]
    parts = [slice(384 * t, 384 * (t + 1)) for t in range(HIDDEN // 384)]
    for cols in tiles:
        for rows in parts:
            u = mm(wit[rows, :], x_ref[:, cols])
            tanh = jnp.tanh(u)
            p = 1.0 + tanh
            h1_ref[rows, cols] = (u * p).astype(jnp.bfloat16)
            s1_ref[rows, cols] = p * (1.0 + u * (1.0 - tanh))
    for cols in tiles:
        for rows in parts:
            u = mm(wmt[rows, :], h1_ref[:, cols])
            back = mm(wot[rows, :], c_ref[:, cols])
            tanh = jnp.tanh(u)
            p = 1.0 + tanh
            h2_ref[rows, cols] = (u * p).astype(jnp.bfloat16)
            d2_ref[rows, cols] = (back * (p * (1.0 + u * (1.0 - tanh)))).astype(jnp.bfloat16)
    for cols in tiles:
        for rows in parts:
            d1_ref[rows, cols] = (mm(wmh[rows, :], d2_ref[:, cols]) * s1_ref[rows, cols]).astype(jnp.bfloat16)
    for cols in tiles:
        grid_ref[band, cols] = mm(wi_ref[...], d1_ref[:, cols]).astype(jnp.bfloat16)
    g1[...] += mm_nt(x_ref[...], d1_ref[...])
    g2[...] += mm_nt(h1_ref[...], d2_ref[...])
    g3[...] += mm_nt(c_ref[...], h2_ref[...])

    @pl.when(n == STEPS - 1)
    def _():
        copies = [
            pltpu.make_async_copy(out_ref.at[:, pl.ds(LANES * t, LANES)], out_hbm.at[:, pl.ds(LANES * t, LANES)], sems.at[t])
            for t in range(TILES)
        ]
        for t in range(TILES):
            out_ref[:, LANES * t : LANES * (t + 1)] = grid_ref[LANES * t : LANES * (t + 1), :].T
            copies[t].start()
        at = 0
        for g in (g1, g2, g3):
            rows = g.shape[0]
            for t in range(HIDDEN // LANES):
                grad_ref[at : at + rows, :] = g[:, LANES * t : LANES * (t + 1)]
                at += rows
        grad_ref[at:, :] = jnp.zeros((GRAD_ROWS * WAYS - at, LANES), jnp.float32)
        for copy in copies:
            copy.wait()


def columns(x, c, wi, wm, wo):
    block = pl.BlockSpec((FEATURES, NLON), lambda n: (0, n))
    kept = pltpu.VMEM((HIDDEN, NLON), jnp.bfloat16)
    return pl.pallas_call(
        column_kernel,
        grid=(STEPS,),
        in_specs=[block, block] + [pl.BlockSpec(w.shape, lambda n: (0, 0)) for w in (wi, wm, wo)],
        out_specs=[
            HBM,
            pl.BlockSpec((GRAD_ROWS * WAYS, LANES), lambda n: (0, 0)),
        ],
        out_shape=[
            jax.ShapeDtypeStruct((NLON, WIDTH), jnp.bfloat16),
            jax.ShapeDtypeStruct((GRAD_ROWS * WAYS, LANES), jnp.float32),
        ],
        scratch_shapes=[
            pltpu.VMEM((HIDDEN, FEATURES), jnp.bfloat16),
            pltpu.VMEM((HIDDEN, HIDDEN), jnp.bfloat16),
            pltpu.VMEM((HIDDEN, FEATURES), jnp.bfloat16),
            pltpu.VMEM((HIDDEN, HIDDEN), jnp.bfloat16),
            kept,
            kept,
            kept,
            kept,
            pltpu.VMEM((HIDDEN, NLON), jnp.float32),
            pltpu.VMEM((WIDTH, NLON), jnp.bfloat16),
            pltpu.VMEM((FEATURES, HIDDEN), jnp.float32),
            pltpu.VMEM((HIDDEN, HIDDEN), jnp.float32),
            pltpu.VMEM((FEATURES, HIDDEN), jnp.float32),
            pltpu.VMEM((NLON, WIDTH), jnp.bfloat16),
            pltpu.SemaphoreType.DMA((TILES,)),
        ],
        compiler_params=params(60),
        name="columns",
    )(x, c, wi, wm, wo)


def wave_kernel(ca_ref, sa_ref, cb_ref, sb_ref, out_ref):
    for s in range(SLOTS):
        rows = slice(WAYS * s, WAYS * (s + 1))
        cb, sb = cb_ref[rows, :], sb_ref[rows, :]
        for a in range(NLON // LANES):
            ca, sa = ca_ref[rows, a : a + 1], sa_ref[rows, a : a + 1]
            cols = slice(LANES * a, LANES * (a + 1))
            out_ref[WAYS * 2 * s : WAYS * (2 * s + 1), cols] = (ca * cb - sa * sb).astype(jnp.bfloat16)
            out_ref[WAYS * (2 * s + 1) : WAYS * (2 * s + 2), cols] = (-(sa * cb + ca * sb)).astype(jnp.bfloat16)


def wave_table(wave_order):
    m = wave_order.reshape(WAYS, SLOTS).T.reshape(NLAT, 1)
    turn = 2.0 * math.pi / NLON
    fine = (m * jnp.arange(LANES, dtype=jnp.int32)[None, :] % NLON).astype(jnp.float32) * turn
    coarse = (m * (LANES * jnp.arange(NLON // LANES, dtype=jnp.int32))[None, :] % NLON).astype(jnp.float32) * turn
    scale = 1.0 / math.sqrt(NLON)
    return pl.pallas_call(
        wave_kernel,
        in_specs=[VMEM] * 4,
        out_specs=VMEM,
        out_shape=jax.ShapeDtypeStruct((NLON, NLON), jnp.bfloat16),
        compiler_params=params(32),
        name="waves",
    )(jnp.cos(coarse), jnp.sin(coarse), jnp.cos(fine) * scale, jnp.sin(fine) * scale)


def legendre_kernel(m_ref, leg_ref, at_ref, as_ref):
    m = m_ref[pl.program_id(0)]
    leg = leg_ref[0]
    row = lax.broadcasted_iota(jnp.int32, (HALF, NLAT), 0)
    col = lax.broadcasted_iota(jnp.int32, (HALF, NLAT), 1)
    lat = 40 * ((col & 127) >> 3) + 8 * (col >> 7) + (col & 7)
    pick = (jnp.where(lat < HALF, lat, NLAT - 1 - lat) == row).astype(jnp.bfloat16)
    full = mm_tn(leg, pick)
    deg = lax.broadcasted_iota(jnp.int32, (NDEG, NLAT), 0)
    col = lax.broadcasted_iota(jnp.int32, (NDEG, NLAT), 1)
    south = (col & 127) >= 64
    full = jnp.where(south & (((deg + m) & 1) == 1), -full, full)
    at_ref[0] = jnp.where(deg >= m, full, 0.0).astype(jnp.bfloat16)
    row = lax.broadcasted_iota(jnp.int32, (NLAT, HALF), 0)
    col = lax.broadcasted_iota(jnp.int32, (NLAT, HALF), 1)
    lat = 5 * (row & 127) + (row >> 7)
    pick = (jnp.where(lat < HALF, lat, NLAT - 1 - lat) == col).astype(jnp.bfloat16)
    full = mm(pick, leg)
    row = lax.broadcasted_iota(jnp.int32, (NLAT, NDEG), 0)
    deg = lax.broadcasted_iota(jnp.int32, (NLAT, NDEG), 1)
    south = (row & 127) >= 64
    full = jnp.where(south & (((deg + m) & 1) == 1), -full, full)
    as_ref[0] = jnp.where(deg >= m, full, 0.0).astype(jnp.bfloat16)


def legendre_tables(wave_local, legendre):
    block = pl.BlockSpec((1, NDEG, NLAT), lambda s, m: (s, 0, 0))
    table = jax.ShapeDtypeStruct((SLOTS, NDEG, NLAT), jnp.bfloat16)
    return pl.pallas_call(
        legendre_kernel,
        grid_spec=pltpu.PrefetchScalarGridSpec(
            num_scalar_prefetch=1,
            grid=(SLOTS,),
            in_specs=[pl.BlockSpec((1, HALF, NDEG), lambda s, m: (s, 0, 0))],
            out_specs=[block, block],
        ),
        out_shape=[table, table],
        compiler_params=params(60),
        name="legendre",
    )(wave_local, legendre)


def group_copies(src, dst, sems):
    return [pltpu.make_async_copy(src.at[pl.ds(GROUP * k, GROUP)], dst.at[pl.ds(GROUP * k, GROUP)], sems.at[k]) for k in range(GROUPS)]


def pack_out(wide_ref, chunk_ref, out_hbm, sems, pitch):
    rows = chunk_ref.shape[1]

    def body(p, carry):
        chunk_ref[p] = wide_ref[pl.ds(pitch * p, rows), :].astype(jnp.bfloat16)
        return carry

    copies = group_copies(chunk_ref, out_hbm, sems)
    for k, copy in enumerate(copies):
        lax.fori_loop(GROUP * k, GROUP * (k + 1), body, 0, unroll=4)
        copy.start()
    for copy in copies:
        copy.wait()


def unpack_in(in_hbm, chunk_ref, wide_ref, sems, pitch, then=()):
    rows = chunk_ref.shape[1]

    def body(p, carry):
        wide_ref[pl.ds(pitch * p, rows), :] = chunk_ref[p].astype(jnp.float32)
        return carry

    copies = group_copies(in_hbm, chunk_ref, sems)
    for copy in (*copies, *then):
        copy.start()
    for k, copy in enumerate(copies):
        copy.wait()
        lax.fori_loop(GROUP * k, GROUP * (k + 1), body, 0, unroll=4)


CHUNKS = pltpu.VMEM((WAYS, ROWS, LANES), jnp.bfloat16)
LATE_CHUNKS = pltpu.VMEM((WAYS, LATE_ROWS, LANES), jnp.bfloat16)
GROUP_SEMS = pltpu.SemaphoreType.DMA((GROUPS,))


def forward_kernel(x_ref, table_ref, grad_ref, out_hbm, wide_ref, chunk_ref, sems):
    def body(k, carry):
        piece = mm(table_ref[pl.ds(pl.multiple_of(256 * k, 256), 256), :], x_ref[...])
        for h in range(2):
            for t in range(TILES):
                wide_ref[pl.ds((2 * k + h) * TILES + t, WAYS, stride=PITCH), :] = piece[
                    WAYS * h : WAYS * (h + 1), LANES * t : LANES * (t + 1)
                ]
        return carry

    lax.fori_loop(0, SLOTS, body, 0)
    for k in range(2):
        wide_ref[pl.ds(DATA_ROWS + k, WAYS, stride=PITCH), :] = jnp.zeros((WAYS, LANES), jnp.float32)
    wide_ref[pl.ds(DATA_ROWS, WAYS, stride=PITCH), :BLOCK_ROWS] = grad_ref[...].T
    pack_out(wide_ref, chunk_ref, out_hbm, sems, PITCH)


def forward(x, table, grad):
    return pl.pallas_call(
        forward_kernel,
        in_specs=[VMEM] * 3,
        out_specs=HBM,
        out_shape=jax.ShapeDtypeStruct((WAYS, ROWS, LANES), jnp.bfloat16),
        scratch_shapes=[pltpu.VMEM((WAYS * PITCH, LANES), jnp.float32), CHUNKS, GROUP_SEMS],
        compiler_params=params(24),
        name="forward",
    )(x, table, grad)


def sum_blocks(wide_ref, sums_ref):
    slab = wide_ref[pl.ds(DATA_ROWS, WAYS, stride=PITCH), :].astype(jnp.bfloat16)
    block = lax.broadcasted_iota(jnp.int32, (BLOCKS, WAYS), 0)
    source = lax.broadcasted_iota(jnp.int32, (BLOCKS, WAYS), 1)
    lat = source >> 3
    owner = ((source & 1) << 4) | ((lat & 1) << 3) | (((lat >> 2) & 1) << 2) | (((lat >> 1) & 1) << 1) | (lat >> 3)
    sums = mm((owner == block).astype(jnp.bfloat16), slab)
    half = BLOCKS // 2
    lane = lax.broadcasted_iota(jnp.int32, (half, LANES), 1)
    sums_ref[:half, :] = jnp.where(lane < 64, sums[:half], pltpu.roll(sums[half:], 64, 1))
    row = lax.broadcasted_iota(jnp.int32, (LANES, LANES), 0)
    col = lax.broadcasted_iota(jnp.int32, (LANES, LANES), 1)
    rest = mm(sums.astype(jnp.bfloat16), (row == 64 + (col & 7)).astype(jnp.bfloat16))
    keep = (lane >> 3) == lax.broadcasted_iota(jnp.int32, (half, LANES), 0)
    for h in range(2):
        part = jnp.where(keep, rest[half * h : half * (h + 1)], 0.0)
        sums_ref[half + h : half + h + 1, :] = jnp.sum(part, axis=0, keepdims=True)


def spectral_kernel(
    m_ref, in_hbm, at_hbm, inv_hbm, as_hbm, out_hbm, wide_ref, chunk_ref, late_ref, x_ref, bank_ref, at_ref, inv_ref, as_ref, sums_ref, sems, group_sems
):
    at_copy = pltpu.make_async_copy(at_hbm, at_ref, sems.at[0])
    inv_copies = []
    for k in range(INV_PARTS):
        part = pl.ds(k * (NDEG // INV_PARTS), NDEG // INV_PARTS)
        inv_copies.append(pltpu.make_async_copy(inv_hbm.at[part], inv_ref.at[part], sems.at[2 + k]))
    as_copy = pltpu.make_async_copy(as_hbm, as_ref, sems.at[1])
    at_copy.start()
    unpack_in(in_hbm, chunk_ref, wide_ref, group_sems, PITCH)
    for copy in inv_copies[:AHEAD]:
        copy.start()
    sum_blocks(wide_ref, sums_ref)
    lane = lax.broadcasted_iota(jnp.int32, (WAYS, LANES), 1)

    def analyse(s, carry):
        for r in range(2):
            tiles = [wide_ref[pl.ds((2 * s + r) * TILES + t, WAYS, stride=PITCH), :] for t in range(TILES)]
            for g in range(2 * SLOTS):
                t, off = divmod(LEVELS * g, LANES)
                piece = tiles[t]
                if off:
                    piece = pltpu.roll(piece, LANES - off, 1)
                    if off + LEVELS > LANES:
                        piece = jnp.where(lane < LANES - off, piece, pltpu.roll(tiles[t + 1], LANES - off, 1))
                i, a = divmod(g, 2)
                x_ref[WAYS * i : WAYS * (i + 1), LANES * (2 * r + a) : LANES * (2 * r + a + 1)] = piece.astype(jnp.bfloat16)
        y = mm(at_ref[s], x_ref[...])
        for j in range(4):
            bank_ref[pl.ds(4 * s + j, NDEG, stride=BANK), :] = y[:, LANES * j : LANES * (j + 1)]
        return carry

    at_copy.wait()
    lax.fori_loop(0, SLOTS, analyse, 0)

    def solve(k, carry):
        for u in range(16):
            deg = 16 * k + u
            rows = pl.ds(deg * BANK, 24)
            bank_ref[rows, :LEVELS] = mm(bank_ref[rows, :LEVELS].astype(jnp.bfloat16), inv_ref[deg])
        return carry

    for copy in (*inv_copies[AHEAD:], as_copy):
        copy.start()
    steps = NDEG // 16 // INV_PARTS
    for k, copy in enumerate(inv_copies):
        copy.wait()
        lax.fori_loop(steps * k, steps * (k + 1), solve, 0)

    def synthesise(s, carry):
        z = jnp.concatenate(
            [bank_ref[pl.ds(4 * s + j, NDEG, stride=BANK), :].astype(jnp.bfloat16) for j in range(4)], axis=1
        )
        weight = jnp.where(m_ref[s] == 0, 1.0, 2.0)
        w = mm(as_ref[s], z) * weight
        for r in range(2):
            tiles = [None] * TILES
            for g in range(2 * SLOTS):
                i, a = divmod(g, 2)
                piece = w[WAYS * i : WAYS * (i + 1), LANES * (2 * r + a) : LANES * (2 * r + a + 1)]
                t, off = divmod(LEVELS * g, LANES)
                if off:
                    piece = pltpu.roll(piece, off, 1)
                tiles[t] = piece if off == 0 else jnp.where(lane < off, tiles[t], piece)
                if off + LEVELS > LANES:
                    tiles[t + 1] = piece
            for t in range(TILES):
                wide_ref[pl.ds((2 * s + r) * TILES + t, WAYS, stride=LATE_PITCH), :] = tiles[t]
        return carry

    as_copy.wait()
    lax.fori_loop(0, SLOTS, synthesise, 0)
    for k in range(GRAD_ROWS):
        row = jnp.broadcast_to(sums_ref[k : k + 1, :], (WAYS, LANES))
        wide_ref[pl.ds(DATA_ROWS + k, WAYS, stride=LATE_PITCH), :] = row
    pack_out(wide_ref, late_ref, out_hbm, group_sems, LATE_PITCH)


def spectral(wave_local, arrived, at, inv, synth):
    return pl.pallas_call(
        spectral_kernel,
        in_specs=[SMEM, ANY, ANY, ANY, ANY],
        out_specs=HBM,
        out_shape=jax.ShapeDtypeStruct((WAYS, LATE_ROWS, LANES), jnp.bfloat16),
        scratch_shapes=[
            pltpu.VMEM((WAYS * LATE_PITCH, LANES), jnp.float32),
            CHUNKS,
            LATE_CHUNKS,
            pltpu.VMEM((NLAT, 4 * LANES), jnp.bfloat16),
            pltpu.VMEM((NDEG * BANK, LANES), jnp.float32),
            pltpu.VMEM((SLOTS, NDEG, NLAT), jnp.bfloat16),
            pltpu.VMEM((NDEG, LEVELS, LEVELS), jnp.bfloat16),
            pltpu.VMEM((SLOTS, NLAT, NDEG), jnp.bfloat16),
            pltpu.VMEM((24, LANES), jnp.float32),
            pltpu.SemaphoreType.DMA((2 + INV_PARTS,)),
            GROUP_SEMS,
        ],
        compiler_params=params(60),
        name="spectral",
    )(wave_local, arrived, at, inv, synth)


def inverse_kernel(in_hbm, table_ref, out_hbm, g1, g2, g3, wide_ref, chunk_ref, rows_ref, out_ref, grad_ref, group_sems, sems):
    unpack_in(in_hbm, chunk_ref, wide_ref, group_sems, LATE_PITCH)
    for t in range(TILES):
        for c in range(2 * SLOTS):
            slab = wide_ref[pl.ds(TILES * c + t, WAYS, stride=LATE_PITCH), :]
            rows_ref[LANES * t : LANES * (t + 1), WAYS * c : WAYS * (c + 1)] = slab.T.astype(jnp.bfloat16)
    copies = []
    for i in range(SLOTS):
        out_ref[i] = mm(rows_ref[FEATURES * i : FEATURES * (i + 1), :], table_ref[...])
        copies.append(pltpu.make_async_copy(out_ref.at[i], out_hbm.at[i], sems.at[i]))
        copies[i].start()
    half = BLOCKS // 2
    for k in range(half):
        both = wide_ref[pl.ds(DATA_ROWS + k, WAYS, stride=LATE_PITCH), :].T
        for h in range(2):
            at = BLOCK_ROWS * (k + half * h)
            grad_ref[at : at + 64, :] = both[64 * h : 64 * (h + 1), :]
    for h in range(2):
        rest = wide_ref[pl.ds(DATA_ROWS + half + h, WAYS, stride=LATE_PITCH), :].T
        for k in range(half):
            at = BLOCK_ROWS * (k + half * h) + 64
            grad_ref[at : at + 8, :] = rest[8 * k : 8 * (k + 1), :]
    scale = 1.0 / math.sqrt(NLAT * NLON)
    at = 0
    for g in (g1, g2, g3):
        rows = g.shape[0]
        for t in range(HIDDEN // LANES):
            g[:, LANES * t : LANES * (t + 1)] = grad_ref[at : at + rows, :] * scale
            at += rows
    for copy in copies:
        copy.wait()


def inverse(arrived, table):
    return pl.pallas_call(
        inverse_kernel,
        in_specs=[ANY, VMEM],
        out_specs=[HBM, VMEM, VMEM, VMEM],
        out_shape=[jax.ShapeDtypeStruct((SLOTS, FEATURES, NLON), jnp.float32)]
        + [jax.ShapeDtypeStruct((r, HIDDEN), jnp.float32) for r in (FEATURES, HIDDEN, FEATURES)],
        scratch_shapes=[
            pltpu.VMEM((WAYS * LATE_PITCH, LANES), jnp.float32),
            LATE_CHUNKS,
            pltpu.VMEM((WIDTH, NLON), jnp.bfloat16),
            pltpu.VMEM((SLOTS, FEATURES, NLON), jnp.float32),
            pltpu.VMEM((GRAD_ROWS * WAYS, LANES), jnp.float32),
            GROUP_SEMS,
            pltpu.SemaphoreType.DMA((SLOTS,)),
        ],
        compiler_params=params(28),
        name="inverse",
    )(arrived, table)


STAGES = (("lev", 1), ("lat", 1), ("lat", 4), ("lat", 2), ("lat", 8))


def across(array, axis, bit):
    size = lax.axis_size(axis)
    return lax.ppermute(array, axis, [(i, i ^ bit) for i in range(size)])


def upper(axis, bit):
    return (lax.axis_index(axis) & bit) != 0


def halve(total, axis, bit):
    half = total.shape[0] // 2
    low, high = total[:half], total[half:]
    mine = upper(axis, bit)
    sent = jnp.where(mine, low, high).astype(jnp.bfloat16)
    return jnp.where(mine, high, low) + across(sent, axis, bit).astype(jnp.float32)


def in_hbm(array):
    return pltpu.with_memory_space_constraint(array, pltpu.HBM)


def swap(array, axis):
    return lax.all_to_all(array, axis, split_axis=0, concat_axis=0, tiled=True)


def program(x, c, wi, wm, wo, legendre, level_inverse, wave_order):
    grid, grad = columns(*map(in_hbm, (x, c, wi, wm, wo)))
    grid, legendre, level_inverse, wave_order = lax.optimization_barrier((grid, legendre, level_inverse, wave_order))
    rows = swap(grid.reshape(8, LONB, WIDTH), "lev")
    rows = rows.reshape(NLON, WIDTH)
    wave_local = lax.dynamic_slice_in_dim(wave_order, lax.axis_index(EVERYWHERE) * SLOTS, SLOTS)
    table = wave_table(wave_order)
    for axis, bit in STAGES:
        grad = halve(grad, axis, bit)
    rows, table, grad = lax.optimization_barrier((rows, table, grad))
    at, synth = legendre_tables(wave_local, legendre)
    inv = level_inverse.transpose(2, 0, 1)
    arrived = swap(forward(rows, table, grad), EVERYWHERE)
    zonal = spectral(wave_local, arrived, at, inv, synth)
    out, g1, g2, g3 = inverse(swap(zonal, EVERYWHERE), table)
    return g1, g2, g3, out.transpose(1, 0, 2)


def solution(mesh):
    in_specs = (
        P(None, EVERYWHERE),
        P(None, EVERYWHERE),
        P(),
        P(),
        P(),
        P(EVERYWHERE, None, None),
        P(),
        P(),
    )
    out_specs = (P(), P(), P(), P(None, EVERYWHERE, None))
    return jax.shard_map(program, mesh=mesh, in_specs=in_specs, out_specs=out_specs, check_vma=False)
```

```python
import math

import jax
import jax.numpy as jnp
from jax import lax
from jax.experimental import pallas as pl
from jax.experimental.pallas import tpu as pltpu
from jax.sharding import PartitionSpec as P


NLAT = 640
NLON = 1280
LEVELS = 88
FEATURES = 176
HIDDEN = 384
NDEG = 640
HALF = NLAT // 2
SLOTS = 5
WAYS = 128
LONB = 160
LANES = 128
WIDTH = 896
TILES = WIDTH // LANES
DATA_ROWS = 2 * SLOTS * TILES
ROWS = 72
LATE_ROWS = 88
GRAD_ROWS = 18
BLOCKS = 32
BLOCK_ROWS = 72
COLS = 6400
TILE = 256
STEPS = COLS // NLON
BANK = 25
INV_PARTS = 5
AHEAD = 3
PITCH = 73
LATE_PITCH = 89
EVERYWHERE = ("lat", "lev")

VMEM = pl.BlockSpec(memory_space=pltpu.VMEM)
SMEM = pl.BlockSpec(memory_space=pltpu.SMEM)
ANY = pl.BlockSpec(memory_space=pl.ANY)
HBM = pl.BlockSpec(memory_space=pltpu.HBM)
GROUPS = 8
GROUP = WAYS // GROUPS


def mm(left, right):
    return jnp.dot(left, right, preferred_element_type=jnp.float32)


def mm_nt(left, right):
    return lax.dot_general(left, right, (((1,), (1,)), ((), ())), preferred_element_type=jnp.float32)


def mm_tn(left, right):
    return lax.dot_general(left, right, (((0,), (0,)), ((), ())), preferred_element_type=jnp.float32)


def params(mib):
    return pltpu.CompilerParams(vmem_limit_bytes=mib * 1024 * 1024)


def column_kernel(x_ref, c_ref, wi_ref, wm_ref, wo_ref, out_hbm, grad_hbm, wit, wmt, wot, wmh, h1_ref, h2_ref, d1_ref, d2_ref, s1_ref, grid_ref, g1, g2, g3, out_ref, grad_ref, sems):
    n = pl.program_id(0)

    @pl.when(n == 0)
    def _():
        half = jnp.bfloat16(0.5)
        wit[...] = wi_ref[...].T * half
        wmt[...] = wm_ref[...].T * half
        wot[...] = wo_ref[...].T * half
        wmh[...] = wm_ref[...] * half
        g1[...] = jnp.zeros_like(g1)
        g2[...] = jnp.zeros_like(g2)
        g3[...] = jnp.zeros_like(g3)
        grid_ref[SLOTS * FEATURES :, :] = jnp.zeros((WIDTH - SLOTS * FEATURES, NLON), jnp.bfloat16)

    band = pl.ds(pl.multiple_of(n * FEATURES, 16), FEATURES)
    tiles = [slice(TILE * t, TILE * (t + 1)) for t in range(NLON // TILE)]
    parts = [slice(384 * t, 384 * (t + 1)) for t in range(HIDDEN // 384)]
    for cols in tiles:
        for rows in parts:
            u = mm(wit[rows, :], x_ref[:, cols])
            tanh = jnp.tanh(u)
            p = 1.0 + tanh
            h1_ref[rows, cols] = (u * p).astype(jnp.bfloat16)
            s1_ref[rows, cols] = p * (1.0 + u * (1.0 - tanh))
    for cols in tiles:
        for rows in parts:
            u = mm(wmt[rows, :], h1_ref[:, cols])
            back = mm(wot[rows, :], c_ref[:, cols])
            tanh = jnp.tanh(u)
            p = 1.0 + tanh
            h2_ref[rows, cols] = (u * p).astype(jnp.bfloat16)
            d2_ref[rows, cols] = (back * (p * (1.0 + u * (1.0 - tanh)))).astype(jnp.bfloat16)
    for cols in tiles:
        for rows in parts:
            d1_ref[rows, cols] = (mm(wmh[rows, :], d2_ref[:, cols]) * s1_ref[rows, cols]).astype(jnp.bfloat16)
    for cols in tiles:
        grid_ref[band, cols] = mm(wi_ref[...], d1_ref[:, cols]).astype(jnp.bfloat16)
    g1[...] += mm_nt(x_ref[...], d1_ref[...])
    g2[...] += mm_nt(h1_ref[...], d2_ref[...])
    g3[...] += mm_nt(c_ref[...], h2_ref[...])

    @pl.when(n == STEPS - 1)
    def _():
        copies = [
            pltpu.make_async_copy(out_ref.at[:, pl.ds(LANES * t, LANES)], out_hbm.at[:, pl.ds(LANES * t, LANES)], sems.at[t])
            for t in range(TILES)
        ]
        at = 0
        for g in (g1, g2, g3):
            rows = g.shape[0]
            for t in range(HIDDEN // LANES):
                grad_ref[at : at + rows, :] = g[:, LANES * t : LANES * (t + 1)]
                at += rows
        grad_ref[at:, :] = jnp.zeros((GRAD_ROWS * WAYS - at, LANES), jnp.float32)
        grad_copy = pltpu.make_async_copy(grad_ref, grad_hbm, sems.at[TILES])
        grad_copy.start()
        for t in range(TILES):
            out_ref[:, LANES * t : LANES * (t + 1)] = grid_ref[LANES * t : LANES * (t + 1), :].T
            copies[t].start()
        grad_copy.wait()
        for copy in copies:
            copy.wait()


def columns(x, c, wi, wm, wo):
    block = pl.BlockSpec((FEATURES, NLON), lambda n: (0, n))
    kept = pltpu.VMEM((HIDDEN, NLON), jnp.bfloat16)
    return pl.pallas_call(
        column_kernel,
        grid=(STEPS,),
        in_specs=[block, block] + [pl.BlockSpec(w.shape, lambda n: (0, 0)) for w in (wi, wm, wo)],
        out_specs=[
            HBM,
            HBM,
        ],
        out_shape=[
            jax.ShapeDtypeStruct((NLON, WIDTH), jnp.bfloat16),
            jax.ShapeDtypeStruct((GRAD_ROWS * WAYS, LANES), jnp.float32),
        ],
        scratch_shapes=[
            pltpu.VMEM((HIDDEN, FEATURES), jnp.bfloat16),
            pltpu.VMEM((HIDDEN, HIDDEN), jnp.bfloat16),
            pltpu.VMEM((HIDDEN, FEATURES), jnp.bfloat16),
            pltpu.VMEM((HIDDEN, HIDDEN), jnp.bfloat16),
            kept,
            kept,
            kept,
            kept,
            pltpu.VMEM((HIDDEN, NLON), jnp.float32),
            pltpu.VMEM((WIDTH, NLON), jnp.bfloat16),
            pltpu.VMEM((FEATURES, HIDDEN), jnp.float32),
            pltpu.VMEM((HIDDEN, HIDDEN), jnp.float32),
            pltpu.VMEM((FEATURES, HIDDEN), jnp.float32),
            pltpu.VMEM((NLON, WIDTH), jnp.bfloat16),
            pltpu.VMEM((GRAD_ROWS * WAYS, LANES), jnp.float32),
            pltpu.SemaphoreType.DMA((TILES + 1,)),
        ],
        compiler_params=params(60),
        name="columns",
    )(x, c, wi, wm, wo)


def wave_kernel(ca_ref, sa_ref, cb_ref, sb_ref, out_ref):
    for s in range(SLOTS):
        rows = slice(WAYS * s, WAYS * (s + 1))
        cb, sb = cb_ref[rows, :], sb_ref[rows, :]
        for a in range(NLON // LANES):
            ca, sa = ca_ref[rows, a : a + 1], sa_ref[rows, a : a + 1]
            cols = slice(LANES * a, LANES * (a + 1))
            out_ref[WAYS * 2 * s : WAYS * (2 * s + 1), cols] = (ca * cb - sa * sb).astype(jnp.bfloat16)
            out_ref[WAYS * (2 * s + 1) : WAYS * (2 * s + 2), cols] = (-(sa * cb + ca * sb)).astype(jnp.bfloat16)


def wave_table(wave_order):
    m = wave_order.reshape(WAYS, SLOTS).T.reshape(NLAT, 1)
    turn = 2.0 * math.pi / NLON
    fine = (m * jnp.arange(LANES, dtype=jnp.int32)[None, :] % NLON).astype(jnp.float32) * turn
    coarse = (m * (LANES * jnp.arange(NLON // LANES, dtype=jnp.int32))[None, :] % NLON).astype(jnp.float32) * turn
    scale = 1.0 / math.sqrt(NLON)
    return pl.pallas_call(
        wave_kernel,
        in_specs=[VMEM] * 4,
        out_specs=VMEM,
        out_shape=jax.ShapeDtypeStruct((NLON, NLON), jnp.bfloat16),
        compiler_params=params(32),
        name="waves",
    )(jnp.cos(coarse), jnp.sin(coarse), jnp.cos(fine) * scale, jnp.sin(fine) * scale)


def legendre_kernel(m_ref, leg_ref, at_ref, as_ref):
    m = m_ref[pl.program_id(0)]
    leg = leg_ref[0]
    row = lax.broadcasted_iota(jnp.int32, (HALF, NLAT), 0)
    col = lax.broadcasted_iota(jnp.int32, (HALF, NLAT), 1)
    lat = 40 * ((col & 127) >> 3) + 8 * (col >> 7) + (col & 7)
    pick = (jnp.where(lat < HALF, lat, NLAT - 1 - lat) == row).astype(jnp.bfloat16)
    full = mm_tn(leg, pick)
    deg = lax.broadcasted_iota(jnp.int32, (NDEG, NLAT), 0)
    col = lax.broadcasted_iota(jnp.int32, (NDEG, NLAT), 1)
    south = (col & 127) >= 64
    full = jnp.where(south & (((deg + m) & 1) == 1), -full, full)
    at_ref[0] = jnp.where(deg >= m, full, 0.0).astype(jnp.bfloat16)
    row = lax.broadcasted_iota(jnp.int32, (NLAT, HALF), 0)
    col = lax.broadcasted_iota(jnp.int32, (NLAT, HALF), 1)
    lat = 5 * (row & 127) + (row >> 7)
    pick = (jnp.where(lat < HALF, lat, NLAT - 1 - lat) == col).astype(jnp.bfloat16)
    full = mm(pick, leg)
    row = lax.broadcasted_iota(jnp.int32, (NLAT, NDEG), 0)
    deg = lax.broadcasted_iota(jnp.int32, (NLAT, NDEG), 1)
    south = (row & 127) >= 64
    full = jnp.where(south & (((deg + m) & 1) == 1), -full, full)
    as_ref[0] = jnp.where(deg >= m, full, 0.0).astype(jnp.bfloat16)


def legendre_tables(wave_local, legendre):
    block = pl.BlockSpec((1, NDEG, NLAT), lambda s, m: (s, 0, 0))
    table = jax.ShapeDtypeStruct((SLOTS, NDEG, NLAT), jnp.bfloat16)
    return pl.pallas_call(
        legendre_kernel,
        grid_spec=pltpu.PrefetchScalarGridSpec(
            num_scalar_prefetch=1,
            grid=(SLOTS,),
            in_specs=[pl.BlockSpec((1, HALF, NDEG), lambda s, m: (s, 0, 0))],
            out_specs=[block, block],
        ),
        out_shape=[table, table],
        compiler_params=params(60),
        name="legendre",
    )(wave_local, legendre)


def group_copies(src, dst, sems):
    return [pltpu.make_async_copy(src.at[pl.ds(GROUP * k, GROUP)], dst.at[pl.ds(GROUP * k, GROUP)], sems.at[k]) for k in range(GROUPS)]


def pack_out(wide_ref, chunk_ref, out_hbm, sems, pitch):
    rows = chunk_ref.shape[1]

    def body(p, carry):
        chunk_ref[p] = wide_ref[pl.ds(pitch * p, rows), :].astype(jnp.bfloat16)
        return carry

    copies = group_copies(chunk_ref, out_hbm, sems)
    for k, copy in enumerate(copies):
        lax.fori_loop(GROUP * k, GROUP * (k + 1), body, 0, unroll=4)
        copy.start()
    for copy in copies:
        copy.wait()


def unpack_in(in_hbm, chunk_ref, wide_ref, sems, pitch, then=()):
    rows = chunk_ref.shape[1]

    def body(p, carry):
        wide_ref[pl.ds(pitch * p, rows), :] = chunk_ref[p].astype(jnp.float32)
        return carry

    copies = group_copies(in_hbm, chunk_ref, sems)
    for copy in (*copies, *then):
        copy.start()
    for k, copy in enumerate(copies):
        copy.wait()
        lax.fori_loop(GROUP * k, GROUP * (k + 1), body, 0, unroll=4)


CHUNKS = pltpu.VMEM((WAYS, ROWS, LANES), jnp.bfloat16)
LATE_CHUNKS = pltpu.VMEM((WAYS, LATE_ROWS, LANES), jnp.bfloat16)
GROUP_SEMS = pltpu.SemaphoreType.DMA((GROUPS,))


def forward_kernel(x_ref, table_ref, grad_ref, out_hbm, wide_ref, chunk_ref, sems):
    def body(k, carry):
        piece = mm(table_ref[pl.ds(pl.multiple_of(256 * k, 256), 256), :], x_ref[...])
        for h in range(2):
            for t in range(TILES):
                wide_ref[pl.ds((2 * k + h) * TILES + t, WAYS, stride=PITCH), :] = piece[
                    WAYS * h : WAYS * (h + 1), LANES * t : LANES * (t + 1)
                ]
        return carry

    lax.fori_loop(0, SLOTS, body, 0)
    for k in range(2):
        wide_ref[pl.ds(DATA_ROWS + k, WAYS, stride=PITCH), :] = jnp.zeros((WAYS, LANES), jnp.float32)
    wide_ref[pl.ds(DATA_ROWS, WAYS, stride=PITCH), :BLOCK_ROWS] = grad_ref[...].T
    pack_out(wide_ref, chunk_ref, out_hbm, sems, PITCH)


def forward(x, table, grad):
    return pl.pallas_call(
        forward_kernel,
        in_specs=[VMEM] * 3,
        out_specs=HBM,
        out_shape=jax.ShapeDtypeStruct((WAYS, ROWS, LANES), jnp.bfloat16),
        scratch_shapes=[pltpu.VMEM((WAYS * PITCH, LANES), jnp.float32), CHUNKS, GROUP_SEMS],
        compiler_params=params(24),
        name="forward",
    )(x, table, grad)


def sum_blocks(wide_ref, sums_ref):
    slab = wide_ref[pl.ds(DATA_ROWS, WAYS, stride=PITCH), :].astype(jnp.bfloat16)
    block = lax.broadcasted_iota(jnp.int32, (BLOCKS, WAYS), 0)
    source = lax.broadcasted_iota(jnp.int32, (BLOCKS, WAYS), 1)
    lat = source >> 3
    owner = ((source & 1) << 4) | ((lat & 1) << 3) | (((lat >> 2) & 1) << 2) | (((lat >> 1) & 1) << 1) | (lat >> 3)
    sums = mm((owner == block).astype(jnp.bfloat16), slab)
    half = BLOCKS // 2
    lane = lax.broadcasted_iota(jnp.int32, (half, LANES), 1)
    sums_ref[:half, :] = jnp.where(lane < 64, sums[:half], pltpu.roll(sums[half:], 64, 1))
    row = lax.broadcasted_iota(jnp.int32, (LANES, LANES), 0)
    col = lax.broadcasted_iota(jnp.int32, (LANES, LANES), 1)
    rest = mm(sums.astype(jnp.bfloat16), (row == 64 + (col & 7)).astype(jnp.bfloat16))
    keep = (lane >> 3) == lax.broadcasted_iota(jnp.int32, (half, LANES), 0)
    for h in range(2):
        part = jnp.where(keep, rest[half * h : half * (h + 1)], 0.0)
        sums_ref[half + h : half + h + 1, :] = jnp.sum(part, axis=0, keepdims=True)


def spectral_kernel(
    m_ref, in_hbm, at_hbm, inv_hbm, as_hbm, out_hbm, wide_ref, chunk_ref, late_ref, x_ref, bank_ref, at_ref, inv_ref, as_ref, sums_ref, sems, group_sems
):
    at_copy = pltpu.make_async_copy(at_hbm, at_ref, sems.at[0])
    inv_copies = []
    for k in range(INV_PARTS):
        part = pl.ds(k * (NDEG // INV_PARTS), NDEG // INV_PARTS)
        inv_copies.append(pltpu.make_async_copy(inv_hbm.at[part], inv_ref.at[part], sems.at[2 + k]))
    as_copy = pltpu.make_async_copy(as_hbm, as_ref, sems.at[1])
    at_copy.start()
    unpack_in(in_hbm, chunk_ref, wide_ref, group_sems, PITCH)
    for copy in inv_copies[:AHEAD]:
        copy.start()
    sum_blocks(wide_ref, sums_ref)
    lane = lax.broadcasted_iota(jnp.int32, (WAYS, LANES), 1)

    def analyse(s, carry):
        for r in range(2):
            tiles = [wide_ref[pl.ds((2 * s + r) * TILES + t, WAYS, stride=PITCH), :] for t in range(TILES)]
            for g in range(2 * SLOTS):
                t, off = divmod(LEVELS * g, LANES)
                piece = tiles[t]
                if off:
                    piece = pltpu.roll(piece, LANES - off, 1)
                    if off + LEVELS > LANES:
                        piece = jnp.where(lane < LANES - off, piece, pltpu.roll(tiles[t + 1], LANES - off, 1))
                i, a = divmod(g, 2)
                x_ref[WAYS * i : WAYS * (i + 1), LANES * (2 * r + a) : LANES * (2 * r + a + 1)] = piece.astype(jnp.bfloat16)
        y = mm(at_ref[s], x_ref[...])
        for j in range(4):
            bank_ref[pl.ds(4 * s + j, NDEG, stride=BANK), :] = y[:, LANES * j : LANES * (j + 1)]
        return carry

    at_copy.wait()
    lax.fori_loop(0, SLOTS, analyse, 0)

    def solve(k, carry):
        for u in range(16):
            deg = 16 * k + u
            rows = pl.ds(deg * BANK, 24)
            bank_ref[rows, :LEVELS] = mm(bank_ref[rows, :LEVELS].astype(jnp.bfloat16), inv_ref[deg])
        return carry

    for copy in (*inv_copies[AHEAD:], as_copy):
        copy.start()
    steps = NDEG // 16 // INV_PARTS
    for k, copy in enumerate(inv_copies):
        copy.wait()
        lax.fori_loop(steps * k, steps * (k + 1), solve, 0)

    def synthesise(s, carry):
        z = jnp.concatenate(
            [bank_ref[pl.ds(4 * s + j, NDEG, stride=BANK), :].astype(jnp.bfloat16) for j in range(4)], axis=1
        )
        weight = jnp.where(m_ref[s] == 0, 1.0, 2.0)
        w = mm(as_ref[s], z) * weight
        for r in range(2):
            tiles = [None] * TILES
            for g in range(2 * SLOTS):
                i, a = divmod(g, 2)
                piece = w[WAYS * i : WAYS * (i + 1), LANES * (2 * r + a) : LANES * (2 * r + a + 1)]
                t, off = divmod(LEVELS * g, LANES)
                if off:
                    piece = pltpu.roll(piece, off, 1)
                tiles[t] = piece if off == 0 else jnp.where(lane < off, tiles[t], piece)
                if off + LEVELS > LANES:
                    tiles[t + 1] = piece
            for t in range(TILES):
                wide_ref[pl.ds((2 * s + r) * TILES + t, WAYS, stride=LATE_PITCH), :] = tiles[t]
        return carry

    as_copy.wait()
    lax.fori_loop(0, SLOTS, synthesise, 0)
    for k in range(GRAD_ROWS):
        row = jnp.broadcast_to(sums_ref[k : k + 1, :], (WAYS, LANES))
        wide_ref[pl.ds(DATA_ROWS + k, WAYS, stride=LATE_PITCH), :] = row
    pack_out(wide_ref, late_ref, out_hbm, group_sems, LATE_PITCH)


def spectral(wave_local, arrived, at, inv, synth):
    return pl.pallas_call(
        spectral_kernel,
        in_specs=[SMEM, ANY, ANY, ANY, ANY],
        out_specs=HBM,
        out_shape=jax.ShapeDtypeStruct((WAYS, LATE_ROWS, LANES), jnp.bfloat16),
        scratch_shapes=[
            pltpu.VMEM((WAYS * LATE_PITCH, LANES), jnp.float32),
            CHUNKS,
            LATE_CHUNKS,
            pltpu.VMEM((NLAT, 4 * LANES), jnp.bfloat16),
            pltpu.VMEM((NDEG * BANK, LANES), jnp.float32),
            pltpu.VMEM((SLOTS, NDEG, NLAT), jnp.bfloat16),
            pltpu.VMEM((NDEG, LEVELS, LEVELS), jnp.bfloat16),
            pltpu.VMEM((SLOTS, NLAT, NDEG), jnp.bfloat16),
            pltpu.VMEM((24, LANES), jnp.float32),
            pltpu.SemaphoreType.DMA((2 + INV_PARTS,)),
            GROUP_SEMS,
        ],
        compiler_params=params(60),
        name="spectral",
    )(wave_local, arrived, at, inv, synth)


def inverse_kernel(in_hbm, table_ref, out_hbm, g1, g2, g3, wide_ref, chunk_ref, rows_ref, out_ref, grad_ref, group_sems, sems):
    unpack_in(in_hbm, chunk_ref, wide_ref, group_sems, LATE_PITCH)
    for t in range(TILES):
        for c in range(2 * SLOTS):
            slab = wide_ref[pl.ds(TILES * c + t, WAYS, stride=LATE_PITCH), :]
            rows_ref[LANES * t : LANES * (t + 1), WAYS * c : WAYS * (c + 1)] = slab.astype(jnp.bfloat16).T
    copies = []
    for i in range(SLOTS):
        out_ref[i] = mm(rows_ref[FEATURES * i : FEATURES * (i + 1), :], table_ref[...])
        copies.append(pltpu.make_async_copy(out_ref.at[i], out_hbm.at[i], sems.at[i]))
        copies[i].start()
    half = BLOCKS // 2
    for k in range(half):
        both = wide_ref[pl.ds(DATA_ROWS + k, WAYS, stride=LATE_PITCH), :].T
        for h in range(2):
            at = BLOCK_ROWS * (k + half * h)
            grad_ref[at : at + 64, :] = both[64 * h : 64 * (h + 1), :]
    for h in range(2):
        rest = wide_ref[pl.ds(DATA_ROWS + half + h, WAYS, stride=LATE_PITCH), :].T
        for k in range(half):
            at = BLOCK_ROWS * (k + half * h) + 64
            grad_ref[at : at + 8, :] = rest[8 * k : 8 * (k + 1), :]
    scale = 1.0 / math.sqrt(NLAT * NLON)
    at = 0
    for g in (g1, g2, g3):
        rows = g.shape[0]
        for t in range(HIDDEN // LANES):
            g[:, LANES * t : LANES * (t + 1)] = grad_ref[at : at + rows, :] * scale
            at += rows
    for copy in copies:
        copy.wait()


def inverse(arrived, table):
    return pl.pallas_call(
        inverse_kernel,
        in_specs=[ANY, VMEM],
        out_specs=[HBM, VMEM, VMEM, VMEM],
        out_shape=[jax.ShapeDtypeStruct((SLOTS, FEATURES, NLON), jnp.float32)]
        + [jax.ShapeDtypeStruct((r, HIDDEN), jnp.float32) for r in (FEATURES, HIDDEN, FEATURES)],
        scratch_shapes=[
            pltpu.VMEM((WAYS * LATE_PITCH, LANES), jnp.float32),
            LATE_CHUNKS,
            pltpu.VMEM((WIDTH, NLON), jnp.bfloat16),
            pltpu.VMEM((SLOTS, FEATURES, NLON), jnp.float32),
            pltpu.VMEM((GRAD_ROWS * WAYS, LANES), jnp.float32),
            GROUP_SEMS,
            pltpu.SemaphoreType.DMA((SLOTS,)),
        ],
        compiler_params=params(28),
        name="inverse",
    )(arrived, table)


STAGES = (("lev", 1), ("lat", 1), ("lat", 4), ("lat", 2), ("lat", 8))


def across(array, axis, bit):
    size = lax.axis_size(axis)
    return lax.ppermute(array, axis, [(i, i ^ bit) for i in range(size)])


def upper(axis, bit):
    return (lax.axis_index(axis) & bit) != 0


def halve(total, axis, bit):
    half = total.shape[0] // 2
    low, high = total[:half], total[half:]
    mine = upper(axis, bit)
    sent = jnp.where(mine, low, high).astype(jnp.bfloat16)
    return jnp.where(mine, high, low) + across(sent, axis, bit).astype(jnp.float32)


def in_hbm(array):
    return pltpu.with_memory_space_constraint(array, pltpu.HBM)


def swap(array, axis):
    return lax.all_to_all(array, axis, split_axis=0, concat_axis=0, tiled=True)


def program(x, c, wi, wm, wo, legendre, level_inverse, wave_order):
    grid, grad = columns(*map(in_hbm, (x, c, wi, wm, wo)))
    grid, legendre, level_inverse, wave_order = lax.optimization_barrier((grid, legendre, level_inverse, wave_order))
    rows = swap(grid.reshape(8, LONB, WIDTH), "lev")
    rows = rows.reshape(NLON, WIDTH)
    wave_local = lax.dynamic_slice_in_dim(wave_order, lax.axis_index(EVERYWHERE) * SLOTS, SLOTS)
    table = wave_table(wave_order)
    for axis, bit in STAGES:
        grad = halve(grad, axis, bit)
    rows, table, grad = lax.optimization_barrier((rows, table, grad))
    at, synth = legendre_tables(wave_local, legendre)
    inv = level_inverse.transpose(2, 0, 1)
    arrived = swap(forward(rows, table, grad), EVERYWHERE)
    zonal = spectral(wave_local, arrived, at, inv, synth)
    out, g1, g2, g3 = inverse(swap(zonal, EVERYWHERE), table)
    return g1, g2, g3, out.transpose(1, 0, 2)


def solution(mesh):
    in_specs = (
        P(None, EVERYWHERE),
        P(None, EVERYWHERE),
        P(),
        P(),
        P(),
        P(EVERYWHERE, None, None),
        P(),
        P(),
    )
    out_specs = (P(), P(), P(), P(None, EVERYWHERE, None))
    return jax.shard_map(program, mesh=mesh, in_specs=in_specs, out_specs=out_specs, check_vma=False)
```
